128 devices in a mesh: seq: 8 (over y, core), head: 16 (over x, z).
Axes of the slice: x: 4, y: 4, z: 4, core: 2. Of those that a mesh axis runs over, the one named last changes fastest.
Arguments:
- queries: bfloat16 [16, 4096, 256], P('head', 'seq'), may hold values from -6 to 6
- keys: bfloat16 [2, 4096, 256], P(None, 'seq'), may hold values from -6 to 6
- values: bfloat16 [2, 4096, 256], P(None, 'seq'), may hold values from -6 to 6
- d_out: bfloat16 [16, 4096, 256], P('head', 'seq'), may hold values from -12 to 12
- doc_lengths: int32 [2, 8], replicated, may hold values from 1 to 1536, 4096 in all within a row
- fold_order: int32 [16], replicated, may hold values from 0 to 15, each once
Outputs:
- grad_queries: bfloat16 [16, 4096, 256], P('head', 'seq')
- grad_keys: float32 [2, 4096, 256], P(None, ('seq', 'head'))
- grad_values: float32 [2, 4096, 256], P(None, ('seq', 'head'))
The draws below stay inside these ranges and needn't reach their ends.
Inputs may be any that keep to these rules, and one draw needn't show every extreme that they name: `doc_lengths`: each row's 8 lengths are at least 1, sum to 4096, and the longest is exactly 1536. fold_order names each of 0 to 15 once.
All inputs are finite; a program needn't handle non-finite values.
Results may differ from the reference program's by a relative error of at most 0.029.
Values may be sent and summed in bfloat16 or wider, within the bound.
A program may use at most 64 MiB of HBM per device.

```python
import math
import jax
import jax.numpy as jnp
import numpy as np

HEAD_COUNT = 8
HEAD_DIM = 256
DOC_COUNT = 8
SEQ_LEN = 4096
BLOCK_LEN = 256
BLOCK_COUNT = 16
PACKED_ROWS = 2
ROW_HEADS = 16
DOC_MOST = 1536


def draw_queries(key, part):
    full_shape = (ROW_HEADS, SEQ_LEN, HEAD_DIM)
    drawn = jnp.clip(jax.random.normal(jax.random.fold_in(key, 3), full_shape, jnp.float32), -6.0, 6.0)
    return drawn.astype(jnp.bfloat16)


def draw_keys(key, part):
    full_shape = (PACKED_ROWS, SEQ_LEN, HEAD_DIM)
    drawn = jnp.clip(jax.random.normal(jax.random.fold_in(key, 5), full_shape, jnp.float32), -6.0, 6.0)
    return drawn.astype(jnp.bfloat16)


def block_levels(key, dims, pieces, smallest, largest):
    factor_of, own = 1.0, jax.random.fold_in(key, 6)
    for dim, blocks in pieces:
        heights = jnp.exp(jax.random.uniform(jax.random.fold_in(own, dim), (blocks,), jnp.float32, smallest / len(pieces), largest / len(pieces)))
        factor_of = factor_of * jnp.repeat(heights, dims[dim] // blocks).reshape([-1 if axis == dim else 1 for axis in range(len(dims))])
    return factor_of


def length_profile(number_of, total, reach, lean):
    loads = [(1 << 20) // math.isqrt(standing ** lean) + 1 for standing in range(2, number_of + 1)]
    spare, counts = total - reach - (number_of - 1), [1] * (number_of - 1)
    while spare > 0:
        candidates = [i for i in range(number_of - 1) if counts[i] < reach]
        whole, budget = sum([loads[i] for i in candidates]), spare
        for i in candidates:
            more = min(reach - counts[i], max(1, budget * loads[i] // whole), spare)
            counts[i] = counts[i] + more
            spare = spare - more
    return np.array([reach] + counts)


def uneven_parts(key, amount, total, most, slope):
    if amount == 2:
        one = jax.random.randint(key, (), max(1, total - most), min(most, total - 1) + 1)
        return jnp.stack([one, total - one])
    tallies = jnp.asarray(length_profile(amount, total, most, slope), jnp.int32)
    pairs = (amount - 1) // 2
    donor, taker = tallies[1:1 + 2 * pairs:2], tallies[2:2 + 2 * pairs:2]
    room = jnp.minimum(donor - 1, most - taker)
    shifted = jax.random.randint(jax.random.fold_in(key, 1), (pairs,), 0, 1 << 20) % (room + 1)
    tallies = tallies.at[1:1 + 2 * pairs:2].set(donor - shifted).at[2:2 + 2 * pairs:2].set(taker + shifted)
    return tallies[jax.random.permutation(jax.random.fold_in(key, 2), amount)]


def bell_draw(stream_key, dims, spread, most, split=(), kind=jnp.bfloat16):
    array = spread * jax.random.normal(stream_key, dims, jnp.float32)
    if split:
        array = array * block_levels(stream_key, dims, split, -0.22, 0.18)
    return jnp.clip(array, -most, most).astype(kind)


def setup_inputs(seed: int = 0) -> dict:
    key_of = jax.random.split(jax.random.key(seed), 7)
    queries = draw_queries(jax.random.fold_in(key_of[6], 71), 0)
    keys = draw_keys(jax.random.fold_in(key_of[6], 71), 0)
    values = bell_draw(key_of[2], (PACKED_ROWS, SEQ_LEN, HEAD_DIM), 1.0, 6.0, ((1, 8),))
    d_out = bell_draw(key_of[3], (ROW_HEADS, SEQ_LEN, HEAD_DIM), 2.0, 12.0, ((0, 16), (1, 8)))
    doc_lengths = jax.vmap(lambda own: uneven_parts(own, DOC_COUNT, SEQ_LEN, DOC_MOST, 2))(jax.random.split(key_of[4], PACKED_ROWS)).reshape((PACKED_ROWS, DOC_COUNT)).astype(jnp.int32)
    fold_order = jax.random.permutation(key_of[5], BLOCK_COUNT).astype(jnp.int32)
    return {"queries": queries, "keys": keys, "values": values, "d_out": d_out, "doc_lengths": doc_lengths, "fold_order": fold_order}


masked_value = -1e30


def reference(queries, keys, values, d_out, doc_lengths, fold_order):
    scaling = HEAD_DIM ** -0.5
    indices = jnp.arange(SEQ_LEN, dtype=jnp.int32)
    position = fold_order[indices // BLOCK_LEN] * BLOCK_LEN + indices % BLOCK_LEN
    query_grads = []
    key_grads = []
    value_grads = []
    for row_index in range(PACKED_ROWS):
        lengths = doc_lengths[row_index]
        starts = jnp.cumsum(lengths, dtype=jnp.int32) - lengths
        document = jnp.sum((position[:, None] >= starts[None, :]).astype(jnp.int32), axis=1, dtype=jnp.int32)
        allowed = (document[:, None] == document[None, :]) & (position[None, :] <= position[:, None])
        key_row = keys[row_index]
        value_row = values[row_index]
        key_total = jnp.zeros((SEQ_LEN, HEAD_DIM), jnp.float32)
        value_total = jnp.zeros((SEQ_LEN, HEAD_DIM), jnp.float32)
        for head_index in range(HEAD_COUNT):
            pair_index = row_index * HEAD_COUNT + head_index
            query_rows = queries[pair_index]
            grad_out = d_out[pair_index]
            scores = jnp.where(allowed, jnp.dot(query_rows, key_row.T, preferred_element_type=jnp.float32) * scaling, masked_value)
            row_max = jnp.max(scores, axis=1, keepdims=True)
            log_norm = row_max + jnp.log(jnp.sum(jnp.exp(scores - row_max), axis=1, keepdims=True))
            weights = jnp.exp(scores - log_norm)
            weights_low = weights.astype(jnp.bfloat16)
            output = jnp.dot(weights_low, value_row, preferred_element_type=jnp.float32)
            grad_dot = jnp.sum(grad_out.astype(jnp.float32) * output, axis=1, keepdims=True)
            grad_prob = jnp.dot(grad_out, value_row.T, preferred_element_type=jnp.float32)
            grad_score = (weights * (grad_prob - grad_dot)).astype(jnp.bfloat16)
            query_grads.append((jnp.dot(grad_score, key_row, preferred_element_type=jnp.float32) * scaling).astype(jnp.bfloat16))
            key_total = key_total + jnp.dot(grad_score.T, query_rows, preferred_element_type=jnp.float32) * scaling
            value_total = value_total + jnp.dot(weights_low.T, grad_out, preferred_element_type=jnp.float32)
        key_grads.append(key_total)
        value_grads.append(value_total)
    return jnp.stack(query_grads), jnp.stack(key_grads), jnp.stack(value_grads)
```

```python
import jax
import jax.numpy as jnp
from jax import lax
from jax.experimental import pallas as pl
from jax.experimental.pallas import tpu as pltpu
from jax.sharding import PartitionSpec as P

MESH = pl.DeviceIdType.MESH
LOG2E = 1.4426950408889634
MASKED = -1e30
BLOCK = 256
F32 = jnp.float32
BF16 = jnp.bfloat16
ROW_HEADS = 8
COPIES = 112


def nt(a, b):
    return lax.dot_general(a, b, (((1,), (1,)), ((), ())), preferred_element_type=F32)


def nn(a, b):
    return lax.dot_general(a, b, (((1,), (0,)), ((), ())), preferred_element_type=F32)


def tn(a, b):
    return lax.dot_general(a, b, (((0,), (0,)), ((), ())), preferred_element_type=F32)


def kernel(
    lengths, fold, q_hbm, k_hbm, v_hbm, do_hbm,
    dq_out, dk_out, dv_out,
    qv, dov, qs, kv, sc, dp, stat, dqt, dqo,
    psend, precv, ak, av, rk, fk, rv, fv, zv, ev, fev, yk, gk, fgk, xs, rx, dkv_out,
    local_sem, send_sem, recv_sem,
):
    s = lax.axis_index("seq")
    h = lax.axis_index("head")
    y, c = lax.div(s, 2), lax.rem(s, 2)
    x, z = lax.div(h, 4), lax.rem(h, 4)
    row = lax.div(h, ROW_HEADS)

    def around(v, k):
        return lax.rem(v + (k % 4), 4)

    partner = {"seq": 2 * y + (1 - c), "head": h}
    yp = {"seq": 2 * around(y, 1) + c, "head": h}
    ym = {"seq": 2 * around(y, -1) + c, "head": h}
    zp = {"seq": s, "head": 4 * x + around(z, 1)}
    zm = {"seq": s, "head": 4 * x + around(z, -1)}
    xo = [{"seq": s, "head": 4 * around(x, k) + z} for k in (1, 2, 3)]

    loads = [
        pltpu.make_async_copy(v_hbm.at[row], kv.at[s, 1], local_sem.at[0]),
        pltpu.make_async_copy(k_hbm.at[row], kv.at[s, 0], local_sem.at[1]),
        pltpu.make_async_copy(q_hbm.at[0], qv, local_sem.at[2]),
        pltpu.make_async_copy(do_hbm.at[0], dov, local_sem.at[3]),
    ]
    for cp in loads:
        cp.start()

    barrier = pltpu.get_barrier_semaphore()
    peers = [partner, yp, ym, zp, zm] + xo
    for peer in peers:
        pl.semaphore_signal(barrier, inc=1, device_id=peer, device_id_type=MESH)
    pl.semaphore_wait(barrier, len(peers))

    started = []

    def send(src, dst, device):
        i = len(started)
        cp = pltpu.make_async_remote_copy(
            src_ref=src, dst_ref=dst, send_sem=send_sem.at[i], recv_sem=recv_sem.at[i],
            device_id=device, device_id_type=MESH,
        )
        cp.start()
        started.append(cp)
        return cp

    def same(ref, device):
        return send(ref, ref, device)

    def sid(k, core):
        return 2 * around(y, k) + core

    other = 1 - c
    zq = 128 * z

    def vquarter(sidx, zi, lo, n):
        return kv.at[sidx, 1, pl.ds(pl.multiple_of(128 * zi + lo, 64), n)]

    loads[0].wait()
    va_p = same(vquarter(s, z, 0, 64), yp)
    vb_m = same(vquarter(s, z, 64, 64), ym)
    vb_p = same(vquarter(s, z, 64, 64), yp)
    va_m = same(vquarter(s, z, 0, 64), ym)
    loads[1].wait()
    ka_p = same(kv.at[s, 0, pl.ds(0, 256)], yp)
    kb_m = same(kv.at[s, 0, pl.ds(256, 256)], ym)
    kb_p = same(kv.at[s, 0, pl.ds(256, 256)], yp)
    ka_m = same(kv.at[s, 0, pl.ds(0, 256)], ym)
    own_pair = same(kv.at[s], partner)

    lane = lax.broadcasted_iota(jnp.int32, (1, 512), 1)
    base0 = fold[2 * s] * BLOCK
    base1 = fold[2 * s + 1] * BLOCK
    pos = jnp.where(lane < BLOCK, base0 + lane, base1 + lane - BLOCK)
    first = jnp.zeros((1, 512), jnp.int32)
    at = jnp.int32(0)
    for d in range(8):
        first = jnp.where(pos >= at, at, first)
        at = at + lengths[row, d]
    loads[2].wait()
    loads[3].wait()
    qs[...] = (qv[...].astype(F32) * 0.0625).astype(BF16)
    stat[0:1, :] = jnp.full((1, 512), MASKED, F32)
    stat[1:2, :] = jnp.zeros((1, 512), F32)
    stat[2:3, :] = jnp.zeros((1, 512), F32)
    rows = lax.broadcasted_iota(jnp.int32, (BLOCK, 512), 0)

    def forward(sidx):
        for half in (0, 1):
            part = pl.ds(half * BLOCK, BLOCK)
            base = fold[2 * sidx + half] * BLOCK
            raw = nt(kv[sidx, 0, part, :], qs[...])
            ok = (rows >= first - base) & (rows <= pos - base)
            s2 = jnp.where(ok, raw * LOG2E, MASKED)
            sc[sidx, part, :] = s2
            gp = nt(kv[sidx, 1, part, :], dov[...])
            dp[sidx, part, :] = gp
            m = stat[0:1, :]
            m_new = jnp.maximum(m, jnp.max(s2, axis=0, keepdims=True))
            alpha = jnp.exp2(m - m_new)
            e = jnp.exp2(s2 - m_new)
            stat[0:1, :] = m_new
            stat[1:2, :] = stat[1:2, :] * alpha + jnp.sum(e, axis=0, keepdims=True)
            stat[2:3, :] = stat[2:3, :] * alpha + jnp.sum(e * gp, axis=0, keepdims=True)

    forward(s)
    va_p.wait_recv()
    v2a = same(vquarter(sid(-1, c), z, 0, 64), yp)
    vb_m.wait_recv()
    v2b = same(vquarter(sid(1, c), z, 64, 64), ym)
    vb_p.wait_recv()
    va_m.wait_recv()
    shares = {}
    for k in (-1, 1):
        shares[k] = (
            same(vquarter(sid(k, c), z, 0, 128), zp),
            same(vquarter(sid(k, c), z, 0, 128), zm),
        )
    own_pair.wait_recv()
    forward(sid(0, other))
    ka_p.wait_recv()
    k2a = same(kv.at[sid(-1, c), 0, pl.ds(0, 256)], yp)
    kb_m.wait_recv()
    k2b = same(kv.at[sid(1, c), 0, pl.ds(256, 256)], ym)

    def relay(k):
        shares[k][0].wait_recv()
        a = same(vquarter(sid(k, c), around(z, -1), 0, 64), zp)
        shares[k][1].wait_recv()
        b = same(vquarter(sid(k, c), around(z, 1), 64, 64), zm)
        return a, b

    v2a.wait_recv()
    v2b.wait_recv()
    shares[2] = (
        same(vquarter(sid(2, c), z, 0, 128), zp),
        same(vquarter(sid(2, c), z, 0, 128), zm),
    )
    relays = {-1: relay(-1), 1: relay(1)}
    kb_p.wait_recv()
    kpair = {-1: same(kv.at[sid(-1, c), 0], partner)}
    ka_m.wait_recv()
    kpair[1] = same(kv.at[sid(1, c), 0], partner)
    relays[2] = relay(2)
    vpair = {}
    for k in (-1, 1):
        for r in relays[k]:
            r.wait_recv()
        vpair[k] = same(kv.at[sid(k, c), 1], partner)
    for k in (-1, 1):
        forward(sid(k, c))
    for r in relays[2]:
        r.wait_recv()
    vpair[2] = same(kv.at[sid(2, c), 1], partner)
    k2a.wait_recv()
    k2b.wait_recv()
    kpair[2] = same(kv.at[sid(2, c), 0], partner)
    for k in (-1, 1):
        kpair[k].wait_recv()
        vpair[k].wait_recv()
        forward(sid(k, other))
    forward(sid(2, c))
    kpair[2].wait_recv()
    vpair[2].wait_recv()
    forward(sid(2, other))

    total = stat[1:2, :]
    lse = stat[0:1, :] + jnp.log2(total)
    gdot = stat[2:3, :] / total

    def backward(sidx, init=False):
        out = []
        for half in (0, 1):
            part = pl.ds(half * BLOCK, BLOCK)
            p = jnp.exp2(sc[sidx, part, :] - lse)
            ds = (p * (dp[sidx, part, :] - gdot)).astype(BF16)
            gv = nn(p.astype(BF16), dov[...])
            gk_ = nn(ds, qs[...])
            add = tn(kv[sidx, 0, part, :], ds)
            if init and half == 0:
                dqt[...] = add
            else:
                dqt[...] += add
            out.append((gk_, gv))
        return out

    def up(v):
        return v.astype(F32)

    offsets = (2, 1, -1, 0)
    pieces = [(xp, zi) for xp in range(4) for zi in range(4)]
    pairs, kc, vc = [], {}, {}

    def values_second(j):
        vc[j, 1].wait_recv()
        zi = around(z, 1)
        av[j, zi, 0:2] = (up(av[j, zi, 0:2]) + up(rv[0, j])).astype(BF16)
        vc[j, 4] = send(av.at[j, zi, pl.ds(0, 2)], fv.at[0, j, pl.ds(0, 2)], zp)
        vc[j, 2].wait_recv()
        zi = around(z, -1)
        av[j, zi, 2:4] = (up(av[j, zi, 2:4]) + up(rv[1, j])).astype(BF16)
        vc[j, 6] = send(av.at[j, zi, pl.ds(2, 2)], fv.at[1, j, pl.ds(2, 2)], zm)

    for j, k in enumerate(offsets):
        for half, (gk_, gv) in enumerate(backward(sid(k, other), j == 0)):
            psend[j, 0, pl.ds(half * BLOCK, BLOCK), :] = gk_.astype(BF16)
            psend[j, 1, pl.ds(half * BLOCK, BLOCK), :] = gv.astype(BF16)
        pairs.append(send(psend.at[j], precv.at[j], partner))
        mine = backward(sid(k, c))
        pairs[j].wait_recv()
        for half, (gk_, gv) in enumerate(mine):
            part = pl.ds(half * BLOCK, BLOCK)
            ak[j, part, :] = (gk_ + up(precv[j, 0, part, :])).astype(BF16)
            gv = (gv + up(precv[j, 1, part, :])).astype(BF16)
            for xp, zi in pieces:
                r0 = (4 * xp + zi) * 32 - half * BLOCK
                if 0 <= r0 < BLOCK:
                    av[j, zi, xp] = gv[r0 : r0 + 32, :]
        if j == 0:
            kc[1] = send(ak.at[0, pl.ds(0, 256)], rk.at[0], yp)
            kc[2] = send(ak.at[0, pl.ds(256, 256)], rk.at[1], ym)
        if j == 1:
            kc[3] = send(ak.at[1, pl.ds(256, 256)], fk.at[0, pl.ds(256, 256)], yp)
        if j == 2:
            kc[5] = send(ak.at[2, pl.ds(0, 256)], fk.at[1, pl.ds(0, 256)], ym)
        vc[j, 1] = send(av.at[j, around(z, 2), pl.ds(0, 2)], rv.at[0, j], zp)
        vc[j, 2] = send(av.at[j, around(z, 2), pl.ds(2, 2)], rv.at[1, j], zm)
        vc[j, 3] = send(av.at[j, around(z, 1), pl.ds(2, 2)], fv.at[0, j, pl.ds(2, 2)], zp)
        vc[j, 5] = send(av.at[j, around(z, -1), pl.ds(0, 2)], fv.at[1, j, pl.ds(0, 2)], zm)
        if j >= 2:
            values_second(j - 2)

    kc[1].wait_recv()
    ak[1, 0:256, :] = (up(ak[1, 0:256, :]) + up(rk[0])).astype(BF16)
    kc[4] = send(ak.at[1, pl.ds(0, 256)], fk.at[0, pl.ds(0, 256)], yp)
    kc[2].wait_recv()
    ak[2, 256:512, :] = (up(ak[2, 256:512, :]) + up(rk[1])).astype(BF16)
    kc[6] = send(ak.at[2, pl.ds(256, 256)], fk.at[1, pl.ds(256, 256)], ym)
    values_second(2)
    values_second(3)

    dqo[...] = (jnp.transpose(dqt[...]) * 0.0625).astype(BF16)
    dq_copy = pltpu.make_async_copy(dqo, dq_out.at[0], local_sem.at[0])
    dq_copy.start()

    def values_first_done(j):
        for i in (3, 4, 5, 6):
            vc[j, i].wait_recv()
        zv[j] = (up(av[j, z]) + up(fv[0, j]) + up(fv[1, j])).astype(BF16)

    ec = {}
    values_first_done(0)
    ec[1] = send(zv.at[0, pl.ds(0, 2)], ev.at[0], yp)
    ec[2] = send(zv.at[0, pl.ds(2, 2)], ev.at[1], ym)
    values_first_done(1)
    ec[3] = send(zv.at[1, pl.ds(2, 2)], fev.at[0, pl.ds(2, 2)], yp)
    values_first_done(2)
    ec[5] = send(zv.at[2, pl.ds(0, 2)], fev.at[1, pl.ds(0, 2)], ym)
    values_first_done(3)

    for i in (3, 4, 5, 6):
        kc[i].wait_recv()
    for xp, zi in pieces:
        r0 = (4 * xp + zi) * 32
        piece = pl.ds(r0, 32)
        yk[zi, xp] = (up(ak[3, piece, :]) + up(fk[0, piece, :]) + up(fk[1, piece, :])).astype(BF16)
    gc = {}
    zi2, zi1, zim = around(z, 2), around(z, 1), around(z, -1)
    gc[1] = send(yk.at[zi2, pl.ds(0, 2)], gk.at[0], zp)
    gc[2] = send(yk.at[zi2, pl.ds(2, 2)], gk.at[1], zm)
    gc[3] = send(yk.at[zi1, pl.ds(2, 2)], fgk.at[0, pl.ds(2, 2)], zp)
    gc[5] = send(yk.at[zim, pl.ds(0, 2)], fgk.at[1, pl.ds(0, 2)], zm)

    ec[1].wait_recv()
    zv[1, 0:2] = (up(zv[1, 0:2]) + up(ev[0])).astype(BF16)
    ec[4] = send(zv.at[1, pl.ds(0, 2)], fev.at[0, pl.ds(0, 2)], yp)
    ec[2].wait_recv()
    zv[2, 2:4] = (up(zv[2, 2:4]) + up(ev[1])).astype(BF16)
    ec[6] = send(zv.at[2, pl.ds(2, 2)], fev.at[1, pl.ds(2, 2)], ym)

    gc[1].wait_recv()
    yk[zi1, 0:2] = (up(yk[zi1, 0:2]) + up(gk[0])).astype(BF16)
    gc[4] = send(yk.at[zi1, pl.ds(0, 2)], fgk.at[0, pl.ds(0, 2)], zp)
    gc[2].wait_recv()
    yk[zim, 2:4] = (up(yk[zim, 2:4]) + up(gk[1])).astype(BF16)
    gc[6] = send(yk.at[zim, pl.ds(2, 2)], fgk.at[1, pl.ds(2, 2)], zm)

    for i in (3, 4, 5, 6):
        ec[i].wait_recv()
    gv = (up(zv[3]) + up(fev[0]) + up(fev[1])).astype(BF16)
    for xp in range(4):
        xs[xp, 1] = gv[xp]
    for i in (3, 4, 5, 6):
        gc[i].wait_recv()
    gk_ = (up(yk[z]) + up(fgk[0]) + up(fgk[1])).astype(BF16)
    for xp in range(4):
        xs[xp, 0] = gk_[xp]
    xc = []
    for k in (1, 2, 3):
        xc.append(send(xs.at[around(x, k)], rx.at[x], xo[k - 1]))
    rx[x] = xs[x]
    for cp in xc:
        cp.wait_recv()
    for r in (0, 1):
        dkv_out[0, r] = up(rx[2 * r, 0]) + up(rx[2 * r + 1, 0])
        dkv_out[1, r] = up(rx[2 * r, 1]) + up(rx[2 * r + 1, 1])
    outs = [
        pltpu.make_async_copy(dkv_out.at[0], dk_out, local_sem.at[1]),
        pltpu.make_async_copy(dkv_out.at[1], dv_out, local_sem.at[2]),
    ]
    for cp in outs:
        cp.start()
    for cp in started:
        cp.wait_send()
    dq_copy.wait()
    for cp in outs:
        cp.wait()


def per_device(queries, keys, values, d_out, doc_lengths, fold_order):
    hbm = pl.BlockSpec(memory_space=pl.ANY)
    smem = pl.BlockSpec(memory_space=pltpu.SMEM)

    def vm(*shape, dtype=BF16):
        return pltpu.VMEM(shape, dtype)

    return pl.pallas_call(
        kernel,
        out_shape=(
            jax.ShapeDtypeStruct((1, 512, 256), BF16),
            jax.ShapeDtypeStruct((2, 32, 256), F32),
            jax.ShapeDtypeStruct((2, 32, 256), F32),
        ),
        in_specs=[smem, smem, hbm, hbm, hbm, hbm],
        out_specs=(hbm, hbm, hbm),
        scratch_shapes=[
            vm(512, 256),
            vm(512, 256),
            vm(512, 256),
            vm(8, 2, 512, 256),
            vm(8, 512, 512, dtype=F32),
            vm(8, 512, 512, dtype=F32),
            vm(8, 512, dtype=F32),
            vm(256, 512, dtype=F32),
            vm(512, 256),
            vm(4, 2, 512, 256),
            vm(4, 2, 512, 256),
            vm(4, 512, 256),
            vm(4, 4, 4, 32, 256),
            vm(2, 256, 256),
            vm(2, 512, 256),
            vm(2, 4, 2, 32, 256),
            vm(2, 4, 4, 32, 256),
            vm(4, 4, 32, 256),
            vm(2, 2, 32, 256),
            vm(2, 4, 32, 256),
            vm(4, 4, 32, 256),
            vm(2, 2, 32, 256),
            vm(2, 4, 32, 256),
            vm(4, 2, 32, 256),
            vm(4, 2, 32, 256),
            vm(2, 2, 32, 256, dtype=F32),
            pltpu.SemaphoreType.DMA((4,)),
            pltpu.SemaphoreType.DMA((COPIES,)),
            pltpu.SemaphoreType.DMA((COPIES,)),
        ],
        compiler_params=pltpu.CompilerParams(
            collective_id=0, has_side_effects=True, vmem_limit_bytes=56 * 1024 * 1024
        ),
    )(doc_lengths, fold_order, queries, keys, values, d_out)


def solution(mesh):
    in_specs = (
        P("head", "seq", None),
        P(None, "seq", None),
        P(None, "seq", None),
        P("head", "seq", None),
        P(),
        P(),
    )
    out_specs = (
        P("head", "seq", None),
        P(None, ("seq", "head"), None),
        P(None, ("seq", "head"), None),
    )
    return jax.shard_map(
        per_device, mesh=mesh, in_specs=in_specs, out_specs=out_specs, check_vma=False
    )
```

```python
import jax
import jax.numpy as jnp
from jax import lax
from jax.experimental import pallas as pl
from jax.experimental.pallas import tpu as pltpu
from jax.sharding import PartitionSpec as P

MESH = pl.DeviceIdType.MESH
LOG2E = 1.4426950408889634
MASKED = -1e30
BLOCK = 256
F32 = jnp.float32
BF16 = jnp.bfloat16
ROW_HEADS = 8
COPIES = 112


def nt(a, b):
    return lax.dot_general(a, b, (((1,), (1,)), ((), ())), preferred_element_type=F32)


def nn(a, b):
    return lax.dot_general(a, b, (((1,), (0,)), ((), ())), preferred_element_type=F32)


def tn(a, b):
    return lax.dot_general(a, b, (((0,), (0,)), ((), ())), preferred_element_type=F32)


def kernel(
    lengths, fold, q_hbm, k_hbm, v_hbm, do_hbm,
    dq_out, dk_out, dv_out,
    qv, dov, qs, kv, sc, dp, stat, dsb, dqt,
    psend, precv, ak, av, rk, fk, rv, fv, zv, ev, fev, yk, gk, fgk, xs, rx,
    local_sem, send_sem, recv_sem,
):
    s = lax.axis_index("seq")
    h = lax.axis_index("head")
    y, c = lax.div(s, 2), lax.rem(s, 2)
    x, z = lax.div(h, 4), lax.rem(h, 4)
    row = lax.div(h, ROW_HEADS)

    def around(v, k):
        return lax.rem(v + (k % 4), 4)

    partner = {"seq": 2 * y + (1 - c), "head": h}
    yp = {"seq": 2 * around(y, 1) + c, "head": h}
    ym = {"seq": 2 * around(y, -1) + c, "head": h}
    zp = {"seq": s, "head": 4 * x + around(z, 1)}
    zm = {"seq": s, "head": 4 * x + around(z, -1)}
    xo = [{"seq": s, "head": 4 * around(x, k) + z} for k in (1, 2, 3)]

    loads = [
        pltpu.make_async_copy(v_hbm.at[row], kv.at[s, 1], local_sem.at[0]),
        pltpu.make_async_copy(k_hbm.at[row], kv.at[s, 0], local_sem.at[1]),
        pltpu.make_async_copy(q_hbm.at[0], qv, local_sem.at[2]),
        pltpu.make_async_copy(do_hbm.at[0], dov, local_sem.at[3]),
    ]
    for cp in loads:
        cp.start()

    barrier = pltpu.get_barrier_semaphore()
    peers = [partner, yp, ym, zp, zm] + xo
    for peer in peers:
        pl.semaphore_signal(barrier, inc=1, device_id=peer, device_id_type=MESH)
    pl.semaphore_wait(barrier, len(peers))

    started = []

    def send(src, dst, device):
        i = len(started)
        cp = pltpu.make_async_remote_copy(
            src_ref=src, dst_ref=dst, send_sem=send_sem.at[i], recv_sem=recv_sem.at[i],
            device_id=device, device_id_type=MESH,
        )
        cp.start()
        started.append(cp)
        return cp

    def same(ref, device):
        return send(ref, ref, device)

    def sid(k, core):
        return 2 * around(y, k) + core

    other = 1 - c
    zq = 128 * z

    def vquarter(sidx, zi, lo, n):
        return kv.at[sidx, 1, pl.ds(pl.multiple_of(128 * zi + lo, 64), n)]

    loads[0].wait()
    va_p = same(vquarter(s, z, 0, 64), yp)
    vb_m = same(vquarter(s, z, 64, 64), ym)
    vb_p = same(vquarter(s, z, 64, 64), yp)
    va_m = same(vquarter(s, z, 0, 64), ym)
    loads[1].wait()
    ka_p = same(kv.at[s, 0, pl.ds(0, 256)], yp)
    kb_m = same(kv.at[s, 0, pl.ds(256, 256)], ym)
    own_pair = same(kv.at[s], partner)

    lane = lax.broadcasted_iota(jnp.int32, (1, 512), 1)
    base0 = fold[2 * s] * BLOCK
    base1 = fold[2 * s + 1] * BLOCK
    pos = jnp.where(lane < BLOCK, base0 + lane, base1 + lane - BLOCK)
    first = jnp.zeros((1, 512), jnp.int32)
    at = jnp.int32(0)
    for d in range(8):
        first = jnp.where(pos >= at, at, first)
        at = at + lengths[row, d]
    loads[2].wait()
    loads[3].wait()
    qs[...] = (qv[...].astype(F32) * 0.0625).astype(BF16)
    stat[0:1, :] = jnp.full((1, 512), MASKED, F32)
    stat[1:2, :] = jnp.zeros((1, 512), F32)
    stat[2:3, :] = jnp.zeros((1, 512), F32)
    rows = lax.broadcasted_iota(jnp.int32, (BLOCK, 512), 0)

    def forward(sidx):
        for half in (0, 1):
            part = pl.ds(half * BLOCK, BLOCK)
            base = fold[2 * sidx + half] * BLOCK
            raw = nt(kv[sidx, 0, part, :], qs[...])
            ok = (rows >= first - base) & (rows <= pos - base)
            s2 = jnp.where(ok, raw * LOG2E, MASKED)
            sc[sidx, part, :] = s2
            gp = nt(kv[sidx, 1, part, :], dov[...])
            dp[sidx, part, :] = gp
            m = stat[0:1, :]
            m_new = jnp.maximum(m, jnp.max(s2, axis=0, keepdims=True))
            alpha = jnp.exp2(m - m_new)
            e = jnp.exp2(s2 - m_new)
            stat[0:1, :] = m_new
            stat[1:2, :] = stat[1:2, :] * alpha + jnp.sum(e, axis=0, keepdims=True)
            stat[2:3, :] = stat[2:3, :] * alpha + jnp.sum(e * gp, axis=0, keepdims=True)

    forward(s)
    va_p.wait_recv()
    v2a = same(vquarter(sid(-1, c), z, 0, 64), yp)
    vb_m.wait_recv()
    v2b = same(vquarter(sid(1, c), z, 64, 64), ym)
    kb_p = same(kv.at[s, 0, pl.ds(256, 256)], yp)
    ka_m = same(kv.at[s, 0, pl.ds(0, 256)], ym)
    vb_p.wait_recv()
    va_m.wait_recv()
    shares = {}
    for k in (-1, 1):
        shares[k] = (
            same(vquarter(sid(k, c), z, 0, 128), zp),
            same(vquarter(sid(k, c), z, 0, 128), zm),
        )
    own_pair.wait_recv()
    forward(sid(0, other))
    ka_p.wait_recv()
    k2a = same(kv.at[sid(-1, c), 0, pl.ds(0, 256)], yp)
    kb_m.wait_recv()
    k2b = same(kv.at[sid(1, c), 0, pl.ds(256, 256)], ym)

    def relay(k):
        shares[k][0].wait_recv()
        a = same(vquarter(sid(k, c), around(z, -1), 0, 64), zp)
        shares[k][1].wait_recv()
        b = same(vquarter(sid(k, c), around(z, 1), 64, 64), zm)
        return a, b

    v2a.wait_recv()
    v2b.wait_recv()
    shares[2] = (
        same(vquarter(sid(2, c), z, 0, 128), zp),
        same(vquarter(sid(2, c), z, 0, 128), zm),
    )
    relays = {-1: relay(-1), 1: relay(1)}
    kb_p.wait_recv()
    kpair = {-1: same(kv.at[sid(-1, c), 0], partner)}
    ka_m.wait_recv()
    kpair[1] = same(kv.at[sid(1, c), 0], partner)
    relays[2] = relay(2)
    vpair = {}
    for k in (-1, 1):
        for r in relays[k]:
            r.wait_recv()
        vpair[k] = same(kv.at[sid(k, c), 1], partner)
    for k in (-1, 1):
        forward(sid(k, c))
    for r in relays[2]:
        r.wait_recv()
    vpair[2] = same(kv.at[sid(2, c), 1], partner)
    k2a.wait_recv()
    k2b.wait_recv()
    kpair[2] = same(kv.at[sid(2, c), 0], partner)
    for k in (-1, 1):
        kpair[k].wait_recv()
        vpair[k].wait_recv()
        forward(sid(k, other))
    forward(sid(2, c))
    kpair[2].wait_recv()
    vpair[2].wait_recv()
    forward(sid(2, other))

    total = stat[1:2, :]
    lse = stat[0:1, :] + jnp.log2(total)
    gdot = stat[2:3, :] / total

    def backward(sidx):
        out = []
        for half in (0, 1):
            part = pl.ds(half * BLOCK, BLOCK)
            p = jnp.exp2(sc[sidx, part, :] - lse)
            ds = (p * (dp[sidx, part, :] - gdot)).astype(BF16)
            dsb[sidx, part, :] = ds
            out.append((nn(ds, qs[...]), nn(p.astype(BF16), dov[...])))
        return out

    def queries(sidxs):
        total = tn(kv[sidxs[0], 0], dsb[sidxs[0]])
        for sidx in sidxs[1:]:
            total = total + tn(kv[sidx, 0], dsb[sidx])
        return total

    def up(v):
        return v.astype(F32)

    offsets = (2, 1, -1, 0)
    pieces = [(xp, zi) for xp in range(4) for zi in range(4)]
    pairs, kc, vc = [], {}, {}

    def values_second(j):
        vc[j, 1].wait_recv()
        zi = around(z, 1)
        av[j, zi, 0:2] = (up(av[j, zi, 0:2]) + up(rv[0, j])).astype(BF16)
        vc[j, 4] = send(av.at[j, zi, pl.ds(0, 2)], fv.at[0, j, pl.ds(0, 2)], zp)
        vc[j, 2].wait_recv()
        zi = around(z, -1)
        av[j, zi, 2:4] = (up(av[j, zi, 2:4]) + up(rv[1, j])).astype(BF16)
        vc[j, 6] = send(av.at[j, zi, pl.ds(2, 2)], fv.at[1, j, pl.ds(2, 2)], zm)

    def theirs(j):
        for half, (gk_, gv) in enumerate(backward(sid(offsets[j], other))):
            psend[j, 0, pl.ds(half * BLOCK, BLOCK), :] = gk_.astype(BF16)
            psend[j, 1, pl.ds(half * BLOCK, BLOCK), :] = gv.astype(BF16)
        pairs.append(send(psend.at[j], precv.at[j], partner))

    def ours(j):
        mine = backward(sid(offsets[j], c))
        pairs[j].wait_recv()
        for half, (gk_, gv) in enumerate(mine):
            part = pl.ds(half * BLOCK, BLOCK)
            ak[j, part, :] = (gk_ + up(precv[j, 0, part, :])).astype(BF16)
            gv = (gv + up(precv[j, 1, part, :])).astype(BF16)
            for xp, zi in pieces:
                r0 = (4 * xp + zi) * 32 - half * BLOCK
                if 0 <= r0 < BLOCK:
                    av[j, zi, xp] = gv[r0 : r0 + 32, :]
        if j == 0:
            kc[1] = send(ak.at[0, pl.ds(0, 256)], rk.at[0], yp)
            kc[2] = send(ak.at[0, pl.ds(256, 256)], rk.at[1], ym)
        if j == 1:
            kc[3] = send(ak.at[1, pl.ds(256, 256)], fk.at[0, pl.ds(256, 256)], yp)
        if j == 2:
            kc[5] = send(ak.at[2, pl.ds(0, 256)], fk.at[1, pl.ds(0, 256)], ym)
        vc[j, 1] = send(av.at[j, around(z, 2), pl.ds(0, 2)], rv.at[0, j], zp)
        vc[j, 2] = send(av.at[j, around(z, 2), pl.ds(2, 2)], rv.at[1, j], zm)
        vc[j, 3] = send(av.at[j, around(z, 1), pl.ds(2, 2)], fv.at[0, j, pl.ds(2, 2)], zp)
        vc[j, 5] = send(av.at[j, around(z, -1), pl.ds(0, 2)], fv.at[1, j, pl.ds(0, 2)], zm)

    theirs(0)
    theirs(1)
    ours(0)
    theirs(2)
    ours(1)
    theirs(3)
    ours(2)
    values_second(0)
    ours(3)
    values_second(1)
    kc[1].wait_recv()
    ak[1, 0:256, :] = (up(ak[1, 0:256, :]) + up(rk[0])).astype(BF16)
    kc[4] = send(ak.at[1, pl.ds(0, 256)], fk.at[0, pl.ds(0, 256)], yp)
    kc[2].wait_recv()
    ak[2, 256:512, :] = (up(ak[2, 256:512, :]) + up(rk[1])).astype(BF16)
    kc[6] = send(ak.at[2, pl.ds(256, 256)], fk.at[1, pl.ds(256, 256)], ym)
    values_second(2)
    values_second(3)

    dqt[...] = queries((0, 1, 2, 3))

    def values_first_done(j):
        for i in (3, 4, 5, 6):
            vc[j, i].wait_recv()
        zv[j] = (up(av[j, z]) + up(fv[0, j]) + up(fv[1, j])).astype(BF16)

    ec = {}
    values_first_done(0)
    ec[1] = send(zv.at[0, pl.ds(0, 2)], ev.at[0], yp)
    ec[2] = send(zv.at[0, pl.ds(2, 2)], ev.at[1], ym)
    values_first_done(1)
    ec[3] = send(zv.at[1, pl.ds(2, 2)], fev.at[0, pl.ds(2, 2)], yp)
    values_first_done(2)
    ec[5] = send(zv.at[2, pl.ds(0, 2)], fev.at[1, pl.ds(0, 2)], ym)
    values_first_done(3)

    for i in (3, 4, 5, 6):
        kc[i].wait_recv()
    for xp, zi in pieces:
        r0 = (4 * xp + zi) * 32
        piece = pl.ds(r0, 32)
        yk[zi, xp] = (up(ak[3, piece, :]) + up(fk[0, piece, :]) + up(fk[1, piece, :])).astype(BF16)
    gc = {}
    zi2, zi1, zim = around(z, 2), around(z, 1), around(z, -1)
    gc[1] = send(yk.at[zi2, pl.ds(0, 2)], gk.at[0], zp)
    gc[2] = send(yk.at[zi2, pl.ds(2, 2)], gk.at[1], zm)
    gc[3] = send(yk.at[zi1, pl.ds(2, 2)], fgk.at[0, pl.ds(2, 2)], zp)
    gc[5] = send(yk.at[zim, pl.ds(0, 2)], fgk.at[1, pl.ds(0, 2)], zm)

    dq_out[0] = (jnp.transpose(dqt[...] + queries((4, 5, 6, 7))) * 0.0625).astype(BF16)
    ec[1].wait_recv()
    zv[1, 0:2] = (up(zv[1, 0:2]) + up(ev[0])).astype(BF16)
    ec[4] = send(zv.at[1, pl.ds(0, 2)], fev.at[0, pl.ds(0, 2)], yp)
    ec[2].wait_recv()
    zv[2, 2:4] = (up(zv[2, 2:4]) + up(ev[1])).astype(BF16)
    ec[6] = send(zv.at[2, pl.ds(2, 2)], fev.at[1, pl.ds(2, 2)], ym)

    gc[1].wait_recv()
    yk[zi1, 0:2] = (up(yk[zi1, 0:2]) + up(gk[0])).astype(BF16)
    gc[4] = send(yk.at[zi1, pl.ds(0, 2)], fgk.at[0, pl.ds(0, 2)], zp)
    gc[2].wait_recv()
    yk[zim, 2:4] = (up(yk[zim, 2:4]) + up(gk[1])).astype(BF16)
    gc[6] = send(yk.at[zim, pl.ds(2, 2)], fgk.at[1, pl.ds(2, 2)], zm)

    for i in (3, 4, 5, 6):
        ec[i].wait_recv()
    gv = (up(zv[3]) + up(fev[0]) + up(fev[1])).astype(BF16)
    for xp in range(4):
        xs[xp, 1] = gv[xp]
    for i in (3, 4, 5, 6):
        gc[i].wait_recv()
    gk_ = (up(yk[z]) + up(fgk[0]) + up(fgk[1])).astype(BF16)
    for xp in range(4):
        xs[xp, 0] = gk_[xp]
    xc = []
    for k in (1, 2, 3):
        xc.append(send(xs.at[around(x, k)], rx.at[x], xo[k - 1]))
    rx[x] = xs[x]
    for cp in xc:
        cp.wait_recv()
    for r in (0, 1):
        dk_out[r] = up(rx[2 * r, 0]) + up(rx[2 * r + 1, 0])
        dv_out[r] = up(rx[2 * r, 1]) + up(rx[2 * r + 1, 1])
    for cp in started:
        cp.wait_send()


def leave(a, b, c, a_out, b_out, c_out, sem):
    moves = [pltpu.make_async_copy(src, dst, sem.at[i]) for i, (src, dst) in enumerate(((a, a_out), (b, b_out), (c, c_out)))]
    for cp in moves:
        cp.start()
    for cp in moves:
        cp.wait()


def per_device(queries, keys, values, d_out, doc_lengths, fold_order):
    hbm = pl.BlockSpec(memory_space=pl.ANY)
    vmem = pl.BlockSpec(memory_space=pltpu.VMEM)
    smem = pl.BlockSpec(memory_space=pltpu.SMEM)

    def vm(*shape, dtype=BF16):
        return pltpu.VMEM(shape, dtype)

    grads = pl.pallas_call(
        kernel,
        out_shape=(
            pltpu.VMEM((1, 512, 256), BF16),
            pltpu.VMEM((2, 32, 256), F32),
            pltpu.VMEM((2, 32, 256), F32),
        ),
        in_specs=[smem, smem, hbm, hbm, hbm, hbm],
        out_specs=(vmem, vmem, vmem),
        scratch_shapes=[
            vm(512, 256),
            vm(512, 256),
            vm(512, 256),
            vm(8, 2, 512, 256),
            vm(8, 512, 512, dtype=F32),
            vm(8, 512, 512, dtype=F32),
            vm(8, 512, dtype=F32),
            vm(8, 512, 512),
            vm(256, 512, dtype=F32),
            vm(4, 2, 512, 256),
            vm(4, 2, 512, 256),
            vm(4, 512, 256),
            vm(4, 4, 4, 32, 256),
            vm(2, 256, 256),
            vm(2, 512, 256),
            vm(2, 4, 2, 32, 256),
            vm(2, 4, 4, 32, 256),
            vm(4, 4, 32, 256),
            vm(2, 2, 32, 256),
            vm(2, 4, 32, 256),
            vm(4, 4, 32, 256),
            vm(2, 2, 32, 256),
            vm(2, 4, 32, 256),
            vm(4, 2, 32, 256),
            vm(4, 2, 32, 256),
            pltpu.SemaphoreType.DMA((4,)),
            pltpu.SemaphoreType.DMA((COPIES,)),
            pltpu.SemaphoreType.DMA((COPIES,)),
        ],
        compiler_params=pltpu.CompilerParams(
            collective_id=0, has_side_effects=True, vmem_limit_bytes=66600000
        ),
    )(doc_lengths, fold_order, queries, keys, values, d_out)
    return pl.pallas_call(
        leave,
        out_shape=tuple(jax.ShapeDtypeStruct(g.shape, g.dtype) for g in grads),
        in_specs=[vmem] * 3,
        out_specs=(hbm,) * 3,
        scratch_shapes=[pltpu.SemaphoreType.DMA((3,))],
        compiler_params=pltpu.CompilerParams(vmem_limit_bytes=1024 * 1024),
    )(*grads)


def solution(mesh):
    in_specs = (
        P("head", "seq", None),
        P(None, "seq", None),
        P(None, "seq", None),
        P("head", "seq", None),
        P(),
        P(),
    )
    out_specs = (
        P("head", "seq", None),
        P(None, ("seq", "head"), None),
        P(None, ("seq", "head"), None),
    )
    return jax.shard_map(
        per_device, mesh=mesh, in_specs=in_specs, out_specs=out_specs, check_vma=False
    )
```

```python
import jax
import jax.numpy as jnp
from jax import lax
from jax.experimental import pallas as pl
from jax.experimental.pallas import tpu as pltpu
from jax.sharding import PartitionSpec as P

MESH = pl.DeviceIdType.MESH
LOG2E = 1.4426950408889634
MASKED = -1e30
BLOCK = 256
F32 = jnp.float32
BF16 = jnp.bfloat16
ROW_HEADS = 8
COPIES = 112
LOW = 256


def nt(a, b):
    return lax.dot_general(a, b, (((1,), (1,)), ((), ())), preferred_element_type=F32)


def nn(a, b):
    return lax.dot_general(a, b, (((1,), (0,)), ((), ())), preferred_element_type=F32)


def tn(a, b):
    return lax.dot_general(a, b, (((0,), (0,)), ((), ())), preferred_element_type=F32)


def kernel(
    lengths, fold, q_hbm, k_hbm, v_hbm, do_hbm,
    dq_out, dk_out, dv_out,
    qv, dov, qs, qst, dot_, kv, sc, dp, stat, stat2, dsb, dqt, dqs, dqr,
    ak, av, rk, fk, dk2, rv, fv, dv2, zv, fev, yk, fgk, xs, rx,
    local_sem, send_sem, recv_sem,
):
    s = lax.axis_index("seq")
    h = lax.axis_index("head")
    y, c = lax.div(s, 2), lax.rem(s, 2)
    x, z = lax.div(h, 4), lax.rem(h, 4)
    row = lax.div(h, ROW_HEADS)

    def around(v, k):
        return lax.rem(v + (k % 4), 4)

    partner = {"seq": 2 * y + (1 - c), "head": h}
    yp = {"seq": 2 * around(y, 1) + c, "head": h}
    ym = {"seq": 2 * around(y, -1) + c, "head": h}
    yf = {"seq": 2 * around(y, 2) + c, "head": h}
    zp = {"seq": s, "head": 4 * x + around(z, 1)}
    zm = {"seq": s, "head": 4 * x + around(z, -1)}
    diag = {
        (i, j): {"seq": 2 * around(y, i) + c, "head": 4 * x + around(z, j)} for i in (-1, 1) for j in (-1, 1)
    }
    xo = [{"seq": s, "head": 4 * around(x, k) + z} for k in (1, 2, 3)]

    mine = pl.ds(pl.multiple_of(512 * c, 512), 512)
    theirs = pl.ds(pl.multiple_of(512 * (1 - c), 512), 512)

    loads = [
        pltpu.make_async_copy(v_hbm.at[row], kv.at[y, 1], local_sem.at[0]),
        pltpu.make_async_copy(k_hbm.at[row], kv.at[y, 0], local_sem.at[1]),
        pltpu.make_async_copy(q_hbm.at[0], qv.at[mine], local_sem.at[2]),
        pltpu.make_async_copy(do_hbm.at[0], dov.at[mine], local_sem.at[3]),
    ]
    for cp in loads:
        cp.start()

    barrier = pltpu.get_barrier_semaphore()
    peers = [partner, yp, ym, yf, zp, zm] + list(diag.values()) + xo
    for peer in peers:
        pl.semaphore_signal(barrier, inc=1, device_id=peer, device_id_type=MESH)
    pl.semaphore_wait(barrier, len(peers))

    started = []

    def send(src, dst, device):
        i = len(started)
        cp = pltpu.make_async_remote_copy(
            src_ref=src, dst_ref=dst, send_sem=send_sem.at[i], recv_sem=recv_sem.at[i],
            device_id=device, device_id_type=MESH,
        )
        cp.start()
        started.append(cp)
        return cp

    def same(ref, device):
        return send(ref, ref, device)

    def chip(k):
        return around(y, k)

    zq = 128 * z

    def vquarter(yi, zi, lo, n):
        return kv.at[yi, 1, pl.ds(pl.multiple_of(128 * zi + lo, 64), n)]

    low, high = pl.ds(0, LOW), pl.ds(LOW, 512 - LOW)
    loads[0].wait()
    v_p = same(vquarter(y, z, 0, 128), yp)
    v_m = same(vquarter(y, z, 0, 128), ym)
    v_f = same(vquarter(y, z, 0, 128), yf)
    loads[1].wait()
    ka_p = same(kv.at[y, 0, low], yp)
    kb_m = same(kv.at[y, 0, high], ym)
    loads[2].wait()
    q_pair = same(qv.at[mine], partner)
    loads[3].wait()
    do_pair = same(dov.at[mine], partner)

    lane = lax.broadcasted_iota(jnp.int32, (1, 1024), 1)
    pos = lane + fold[4 * y] * BLOCK
    for b in (1, 2, 3):
        pos = jnp.where(lane < BLOCK * b, pos, lane + (fold[4 * y + b] - b) * BLOCK)
    first = jnp.zeros((1, 1024), jnp.int32)
    at = jnp.int32(0)
    for d in range(8):
        first = jnp.where(pos >= at, at, first)
        at = at + lengths[row, d]
    rows = lax.broadcasted_iota(jnp.int32, (BLOCK, 1024), 0)
    stat[0:1, :] = jnp.full((1, 1024), MASKED, F32)
    stat[1:3, :] = jnp.zeros((2, 1024), F32)
    stat[3:4, :] = jnp.full((1, 1024), MASKED, F32)
    stat[4:8, :] = jnp.zeros((4, 1024), F32)
    q_pair.wait_recv()
    qs[...] = (qv[...].astype(F32) * 0.0625).astype(BF16)
    qst[...] = jnp.transpose(qs[...])
    do_pair.wait_recv()
    dot_[...] = jnp.transpose(dov[...])

    offsets = (2, 1, -1, 0)

    parts = [pl.ds(half * BLOCK, BLOCK) for half in (0, 1)]

    def scores(j):
        yi = chip(offsets[j])
        m = stat[0:1, :]
        for half, part in enumerate(parts):
            base = fold[4 * yi + 2 * c + half] * BLOCK
            raw = nn(kv[yi, 0, part, :], qst[...])
            ok = (rows >= first - base) & (rows <= pos - base)
            s2 = jnp.where(ok, raw * LOG2E, MASKED)
            sc[j, part, :] = s2
            m = jnp.maximum(m, jnp.max(s2, axis=0, keepdims=True))
        stat[0:1, :] = m

    def probs(j):
        yi = chip(offsets[j])
        m = stat[0:1, :]
        alpha = jnp.exp2(stat[3:4, :] - m)
        total = stat[1:2, :] * alpha
        dot = stat[2:3, :] * alpha
        for part in parts:
            gp = nn(kv[yi, 1, part, :], dot_[...])
            dp[j, part, :] = gp
            e = jnp.exp2(sc[j, part, :] - m)
            total = total + jnp.sum(e, axis=0, keepdims=True)
            dot = dot + jnp.sum(e * gp, axis=0, keepdims=True)
        stat[1:2, :] = total
        stat[2:3, :] = dot
        stat[3:4, :] = m

    shares, relays = {}, {}

    def share(k):
        shares[k] = (
            same(vquarter(chip(k), z, 0, 128), zp),
            same(vquarter(chip(k), z, 0, 128), zm),
        )

    def relay(k):
        shares[k][0].wait_recv()
        a = same(vquarter(chip(k), around(z, -1), 0, 64), zp)
        shares[k][1].wait_recv()
        relays[k] = a, same(vquarter(chip(k), around(z, 1), 64, 64), zm)

    v_p.wait_recv()
    share(-1)
    v_m.wait_recv()
    share(1)
    kb_p = same(kv.at[y, 0, high], yp)
    ka_m = same(kv.at[y, 0, low], ym)
    v_f.wait_recv()
    share(2)
    ka_p.wait_recv()
    k2a = same(kv.at[chip(-1), 0, low], yp)
    kb_m.wait_recv()
    k2b = same(kv.at[chip(1), 0, high], ym)
    scores(3)
    probs(3)
    relay(-1)
    relay(1)
    kb_p.wait_recv()
    ka_m.wait_recv()
    scores(1)
    relay(2)
    scores(2)
    for k in (-1, 1):
        for r in relays[k]:
            r.wait_recv()
    probs(1)
    probs(2)
    k2a.wait_recv()
    k2b.wait_recv()
    scores(0)
    for r in relays[2]:
        r.wait_recv()
    probs(0)

    stat_pair = send(stat, stat2, partner)
    stat_pair.wait_recv()
    top = jnp.maximum(stat[0:1, :], stat2[0:1, :])
    w1 = jnp.exp2(stat[0:1, :] - top)
    w2 = jnp.exp2(stat2[0:1, :] - top)
    total = stat[1:2, :] * w1 + stat2[1:2, :] * w2
    lse = top + jnp.log2(total)
    gdot = (stat[2:3, :] * w1 + stat2[2:3, :] * w2) / total

    def backward(j):
        out = []
        for half in (0, 1):
            part = pl.ds(half * BLOCK, BLOCK)
            p = jnp.exp2(sc[j, part, :] - lse)
            ds = (p * (dp[j, part, :] - gdot)).astype(BF16)
            dsb[j, part, :] = ds
            out.append((nn(ds, qs[...]), nn(p.astype(BF16), dov[...])))
        return out

    def queries():
        acc = tn(kv[chip(offsets[0]), 0], dsb[0])
        for j in (1, 2, 3):
            acc = acc + tn(kv[chip(offsets[j]), 0], dsb[j])
        return acc

    def up(v):
        return v.astype(F32)

    pieces = [(xp, zi) for xp in range(4) for zi in range(4)]
    place = [lax.rem(zi - z + 5, 4) for zi in range(4)]
    lo, hi = pl.ds(0, 2), pl.ds(2, 2)
    near, far = pl.ds(0, 3), 3
    kc, vc = {}, {}

    def values_second(j):
        vc[j, 1].wait_recv()
        av[j, 2, 0:2] = (up(av[j, 2, 0:2]) + up(rv[0, j])).astype(BF16)
        if j == 0:
            vc[j, 4] = send(av.at[j, 2, lo], dv2.at[0, 0], diag[1, 1])
        else:
            vc[j, 4] = send(av.at[j, 2, lo], fv.at[0, j, lo], zp)
        vc[j, 2].wait_recv()
        av[j, 0, 2:4] = (up(av[j, 0, 2:4]) + up(rv[1, j])).astype(BF16)
        if j == 0:
            vc[j, 6] = send(av.at[j, 0, hi], dv2.at[1, 0], diag[-1, -1])
        else:
            vc[j, 6] = send(av.at[j, 0, hi], fv.at[1, j, hi], zm)

    def values_early():
        vc[0, 5].wait_recv()
        av[0, 1, 0:2] = (up(av[0, 1, 0:2]) + up(fv[1, 0, 0:2])).astype(BF16)
        vc[0, 7] = send(av.at[0, 1, lo], dv2.at[0, 1], yp)
        vc[0, 3].wait_recv()
        av[0, 1, 2:4] = (up(av[0, 1, 2:4]) + up(fv[0, 0, 2:4])).astype(BF16)
        vc[0, 8] = send(av.at[0, 1, hi], dv2.at[1, 1], ym)

    def keys_early():
        kc[5].wait_recv()
        ak[3, 3, 0:2] = (up(ak[3, 3, 0:2]) + up(fk[1, 3, 0:2])).astype(BF16)
        kc[17] = send(ak.at[3, far, lo], dk2.at[0, 1], zp)
        kc[3].wait_recv()
        ak[3, 3, 2:4] = (up(ak[3, 3, 2:4]) + up(fk[0, 3, 2:4])).astype(BF16)
        kc[18] = send(ak.at[3, far, hi], dk2.at[1, 1], zm)

    def block(j):
        for half, (gk_, gv) in enumerate(backward(j)):
            gk_, gv = gk_.astype(BF16), gv.astype(BF16)
            for xp, zi in pieces:
                r0 = (4 * xp + zi) * 32 - half * BLOCK
                if 0 <= r0 < BLOCK:
                    ak[j, place[zi], xp] = gk_[r0 : r0 + 32, :]
                    av[j, place[zi], xp] = gv[r0 : r0 + 32, :]
        for half in (0, 1):
            at_ = (lo, hi)[half]
            to = (zp, zm)[half]
            vc[j, 1 + half] = send(av.at[j, far, at_], rv.at[half, j], to)
            if j == 0:
                kc[1 + half] = send(ak.at[0, pl.ds(0, 4), at_], rk.at[half], (yp, ym)[half])
            if j == 1 and half == 1:
                kc[3] = send(ak.at[1, pl.ds(0, 4), hi], fk.at[0, pl.ds(0, 4), hi], yp)
            if j == 2 and half == 0:
                kc[5] = send(ak.at[2, pl.ds(0, 4), lo], fk.at[1, pl.ds(0, 4), lo], ym)
            if half == 0:
                vc[j, 5] = send(av.at[j, 0, lo], fv.at[1, j, lo], zm)
            else:
                vc[j, 3] = send(av.at[j, 2, hi], fv.at[0, j, hi], zp)

    block(0)
    block(1)
    block(2)
    values_second(0)
    block(3)
    values_early()
    values_second(1)
    kc[1].wait_recv()
    ak[1, :, 0:2] = (up(ak[1, :, 0:2]) + up(rk[0])).astype(BF16)
    kc[14] = send(ak.at[1, far, lo], dk2.at[0, 0], diag[1, 1])
    kc[4] = send(ak.at[1, near, lo], fk.at[0, pl.ds(0, 3), lo], yp)
    kc[2].wait_recv()
    ak[2, :, 2:4] = (up(ak[2, :, 2:4]) + up(rk[1])).astype(BF16)
    kc[16] = send(ak.at[2, far, hi], dk2.at[1, 0], diag[-1, -1])
    kc[6] = send(ak.at[2, near, hi], fk.at[1, pl.ds(0, 3), hi], ym)
    values_second(2)
    values_second(3)

    keys_early()
    dqt[...] = queries()
    dqs[...] = jnp.transpose(dqt[:, theirs])
    dq_pair = send(dqs, dqr, partner)

    def values_along_z(j):
        for i in (3, 4, 5, 6):
            vc[j, i].wait_recv()
        return up(av[j, 1]) + up(fv[0, j]) + up(fv[1, j])

    for i in (4, 6, 7, 8):
        vc[0, i].wait_recv()
    ec = {}
    w = values_along_z(1)
    zv[0, 0:2] = (w[0:2] + up(dv2[0, 0]) + up(dv2[0, 1])).astype(BF16)
    zv[0, 2:4] = w[2:4].astype(BF16)
    ec[0] = send(zv.at[0], fev.at[0], yp)
    w = values_along_z(2)
    zv[1, 0:2] = w[0:2].astype(BF16)
    zv[1, 2:4] = (w[2:4] + up(dv2[1, 0]) + up(dv2[1, 1])).astype(BF16)
    ec[1] = send(zv.at[1], fev.at[1], ym)

    for i in (4, 6):
        kc[i].wait_recv()

    def keys_along_y(q):
        return up(ak[3, q]) + up(fk[0, q]) + up(fk[1, q])

    for i in (14, 16, 17, 18):
        kc[i].wait_recv()
    gc = {}
    w = keys_along_y(2)
    yk[0, 0:2] = (w[0:2] + up(dk2[0, 0]) + up(dk2[0, 1])).astype(BF16)
    yk[0, 2:4] = w[2:4].astype(BF16)
    gc[0] = send(yk.at[0], fgk.at[0], zp)
    w = keys_along_y(0)
    yk[1, 0:2] = w[0:2].astype(BF16)
    yk[1, 2:4] = (w[2:4] + up(dk2[1, 0]) + up(dk2[1, 1])).astype(BF16)
    gc[1] = send(yk.at[1], fgk.at[1], zm)

    w = values_along_z(3)
    for cp in ec.values():
        cp.wait_recv()
    xs[1] = (w + up(fev[0]) + up(fev[1])).astype(BF16)
    xc = []
    for k in (1, 2, 3):
        xc.append(send(xs.at[1, around(x, k)], rx.at[1, x], xo[k - 1]))
    dq_pair.wait_recv()
    dq_out[0] = ((jnp.transpose(dqt[:, mine]) + dqr[...]) * 0.0625).astype(BF16)
    for cp in gc.values():
        cp.wait_recv()
    xs[0] = (keys_along_y(1) + up(fgk[0]) + up(fgk[1])).astype(BF16)
    for k in (1, 2, 3):
        xc.append(send(xs.at[0, around(x, k)], rx.at[0, x], xo[k - 1]))
    rx[0, x] = xs[0, x]
    rx[1, x] = xs[1, x]
    for cp in xc:
        cp.wait_recv()
    for r in (0, 1):
        dk_out[r] = up(rx[0, 2 * r]) + up(rx[0, 2 * r + 1])
        dv_out[r] = up(rx[1, 2 * r]) + up(rx[1, 2 * r + 1])
    for cp in started:
        cp.wait_send()


def leave(a, b, c, a_out, b_out, c_out, sem):
    moves = [pltpu.make_async_copy(src, dst, sem.at[i]) for i, (src, dst) in enumerate(((a, a_out), (b, b_out), (c, c_out)))]
    for cp in moves:
        cp.start()
    for cp in moves:
        cp.wait()


def per_device(queries, keys, values, d_out, doc_lengths, fold_order):
    hbm = pl.BlockSpec(memory_space=pl.ANY)
    vmem = pl.BlockSpec(memory_space=pltpu.VMEM)
    smem = pl.BlockSpec(memory_space=pltpu.SMEM)

    def vm(*shape, dtype=BF16):
        return pltpu.VMEM(shape, dtype)

    grads = pl.pallas_call(
        kernel,
        out_shape=(
            pltpu.VMEM((1, 512, 256), BF16),
            pltpu.VMEM((2, 32, 256), F32),
            pltpu.VMEM((2, 32, 256), F32),
        ),
        in_specs=[smem, smem, hbm, hbm, hbm, hbm],
        out_specs=(vmem, vmem, vmem),
        scratch_shapes=[
            vm(1024, 256),
            vm(1024, 256),
            vm(1024, 256),
            vm(256, 1024),
            vm(256, 1024),
            vm(4, 2, 512, 256),
            vm(4, 512, 1024, dtype=F32),
            vm(4, 512, 1024, dtype=F32),
            vm(8, 1024, dtype=F32),
            vm(8, 1024, dtype=F32),
            vm(4, 512, 1024),
            vm(256, 1024, dtype=F32),
            vm(512, 256, dtype=F32),
            vm(512, 256, dtype=F32),
            vm(4, 4, 4, 32, 256),
            vm(4, 4, 4, 32, 256),
            vm(2, 4, 2, 32, 256),
            vm(2, 4, 4, 32, 256),
            vm(2, 2, 2, 32, 256),
            vm(2, 4, 2, 32, 256),
            vm(2, 4, 4, 32, 256),
            vm(2, 2, 2, 32, 256),
            vm(2, 4, 32, 256),
            vm(2, 4, 32, 256),
            vm(2, 4, 32, 256),
            vm(2, 4, 32, 256),
            vm(2, 4, 32, 256),
            vm(2, 4, 32, 256),
            pltpu.SemaphoreType.DMA((4,)),
            pltpu.SemaphoreType.DMA((COPIES,)),
            pltpu.SemaphoreType.DMA((COPIES,)),
        ],
        compiler_params=pltpu.CompilerParams(
            collective_id=0, has_side_effects=True, vmem_limit_bytes=66600000
        ),
    )(doc_lengths, fold_order, queries, keys, values, d_out)
    return pl.pallas_call(
        leave,
        out_shape=tuple(jax.ShapeDtypeStruct(g.shape, g.dtype) for g in grads),
        in_specs=[vmem] * 3,
        out_specs=(hbm,) * 3,
        scratch_shapes=[pltpu.SemaphoreType.DMA((3,))],
        compiler_params=pltpu.CompilerParams(vmem_limit_bytes=1024 * 1024),
    )(*grads)


def solution(mesh):
    in_specs = (
        P("head", "seq", None),
        P(None, "seq", None),
        P(None, "seq", None),
        P("head", "seq", None),
        P(),
        P(),
    )
    out_specs = (
        P("head", "seq", None),
        P(None, ("seq", "head"), None),
        P(None, ("seq", "head"), None),
    )
    return jax.shard_map(
        per_device, mesh=mesh, in_specs=in_specs, out_specs=out_specs, check_vma=False
    )
```

```python
import jax
import jax.numpy as jnp
from jax import lax
from jax.experimental import pallas as pl
from jax.experimental.pallas import tpu as pltpu
from jax.sharding import PartitionSpec as P

MESH = pl.DeviceIdType.MESH
LOG2E = 1.4426950408889634
MASKED = -1e30
BLOCK = 256
F32 = jnp.float32
BF16 = jnp.bfloat16
ROW_HEADS = 8
COPIES = 71
SENDS = 40
LOW = 256


def nt(a, b):
    return lax.dot_general(a, b, (((1,), (1,)), ((), ())), preferred_element_type=F32)


def nn(a, b):
    return lax.dot_general(a, b, (((1,), (0,)), ((), ())), preferred_element_type=F32)


def tn(a, b):
    return lax.dot_general(a, b, (((0,), (0,)), ((), ())), preferred_element_type=F32)


def kernel(
    lengths, fold, q_hbm, k_hbm, v_hbm, do_hbm,
    dq_out, dk_out, dv_out,
    qv, dov, qs, qst, dot_, kv, sc, dp, stat, stat2, dsb, dqt, dqs, dqr,
    ak, av, rk, fk, dk2, rv, fv, dv2, zv, fev, yk, fgk, xs, rx,
    local_sem, send_sem, recv_sem,
):
    s = lax.axis_index("seq")
    h = lax.axis_index("head")
    y, c = lax.div(s, 2), lax.rem(s, 2)
    x, z = lax.div(h, 4), lax.rem(h, 4)
    row = lax.div(h, ROW_HEADS)

    def around(v, k):
        return lax.rem(v + (k % 4), 4)

    partner = {"seq": 2 * y + (1 - c), "head": h}
    yp = {"seq": 2 * around(y, 1) + c, "head": h}
    ym = {"seq": 2 * around(y, -1) + c, "head": h}
    yf = {"seq": 2 * around(y, 2) + c, "head": h}
    zp = {"seq": s, "head": 4 * x + around(z, 1)}
    zm = {"seq": s, "head": 4 * x + around(z, -1)}
    diag = {
        (i, j): {"seq": 2 * around(y, i) + c, "head": 4 * x + around(z, j)} for i in (-1, 1) for j in (-1, 1)
    }
    xo = [{"seq": s, "head": 4 * around(x, k) + z} for k in (1, 2, 3)]

    mine = pl.ds(pl.multiple_of(512 * c, 512), 512)
    theirs = pl.ds(pl.multiple_of(512 * (1 - c), 512), 512)

    loads = [
        pltpu.make_async_copy(v_hbm.at[row], kv.at[y, 1], local_sem.at[0]),
        pltpu.make_async_copy(k_hbm.at[row], kv.at[y, 0], local_sem.at[1]),
        pltpu.make_async_copy(q_hbm.at[0], qv.at[mine], local_sem.at[2]),
        pltpu.make_async_copy(do_hbm.at[0], dov.at[mine], local_sem.at[3]),
    ]
    for cp in loads:
        cp.start()

    barrier = pltpu.get_barrier_semaphore()
    peers = [partner, yp, ym, yf, zp, zm] + list(diag.values()) + xo
    for peer in peers:
        pl.semaphore_signal(barrier, inc=1, device_id=peer, device_id_type=MESH)
    pl.semaphore_wait(barrier, len(peers))

    started = []

    def send(src, dst, device):
        i = len(started)
        if i >= SENDS:
            started[i - SENDS].wait_send()
        cp = pltpu.make_async_remote_copy(
            src_ref=src, dst_ref=dst, send_sem=send_sem.at[i % SENDS], recv_sem=recv_sem.at[i],
            device_id=device, device_id_type=MESH,
        )
        cp.start()
        started.append(cp)
        return cp

    def same(ref, device):
        return send(ref, ref, device)

    def chip(k):
        return around(y, k)

    zq = 128 * z

    def vquarter(yi, zi, lo, n):
        return kv.at[yi, 1, pl.ds(pl.multiple_of(128 * zi + lo, 64), n)]

    low, high = pl.ds(0, LOW), pl.ds(LOW, 512 - LOW)
    loads[0].wait()
    v_p = same(vquarter(y, z, 0, 128), yp)
    v_m = same(vquarter(y, z, 0, 128), ym)
    v_f = same(vquarter(y, z, 0, 128), yf)
    loads[2].wait()
    q_pair = same(qv.at[mine], partner)
    loads[3].wait()
    do_pair = same(dov.at[mine], partner)

    lane = lax.broadcasted_iota(jnp.int32, (1, 1024), 1)
    pos = lane + fold[4 * y] * BLOCK
    for b in (1, 2, 3):
        pos = jnp.where(lane < BLOCK * b, pos, lane + (fold[4 * y + b] - b) * BLOCK)
    first = jnp.zeros((1, 1024), jnp.int32)
    at = jnp.int32(0)
    for d in range(8):
        first = jnp.where(pos >= at, at, first)
        at = at + lengths[row, d]
    rows = lax.broadcasted_iota(jnp.int32, (BLOCK, 1024), 0)
    stat[0:1, :] = jnp.full((1, 1024), MASKED, F32)
    stat[1:3, :] = jnp.zeros((2, 1024), F32)
    stat[3:4, :] = jnp.full((1, 1024), MASKED, F32)
    stat[4:8, :] = jnp.zeros((4, 1024), F32)
    q_pair.wait_recv()
    qs[...] = (qv[...].astype(F32) * 0.0625).astype(BF16)
    qst[...] = jnp.transpose(qs[...])
    do_pair.wait_recv()
    dot_[...] = jnp.transpose(dov[...])

    offsets = (2, 1, -1, 0)

    parts = [pl.ds(half * BLOCK, BLOCK) for half in (0, 1)]

    def scores(j, halves=(0, 1)):
        yi = chip(offsets[j])
        m = stat[0:1, :]
        for half in halves:
            part = parts[half]
            base = fold[4 * yi + 2 * c + half] * BLOCK
            raw = nn(kv[yi, 0, part, :], qst[...])
            ok = (rows >= first - base) & (rows <= pos - base)
            s2 = jnp.where(ok, raw * LOG2E, MASKED)
            sc[j, part, :] = s2
            m = jnp.maximum(m, jnp.max(s2, axis=0, keepdims=True))
        stat[0:1, :] = m

    def probs(j):
        yi = chip(offsets[j])
        m = stat[0:1, :]
        alpha = jnp.exp2(stat[3:4, :] - m)
        total = stat[1:2, :] * alpha
        dot = stat[2:3, :] * alpha
        for part in parts:
            gp = nn(kv[yi, 1, part, :], dot_[...])
            dp[j, part, :] = gp
            e = jnp.exp2(sc[j, part, :] - m)
            total = total + jnp.sum(e, axis=0, keepdims=True)
            dot = dot + jnp.sum(e * gp, axis=0, keepdims=True)
        stat[1:2, :] = total
        stat[2:3, :] = dot
        stat[3:4, :] = m

    shares, relays = {}, {}

    def share(k):
        shares[k] = (
            same(vquarter(chip(k), z, 0, 128), zp),
            same(vquarter(chip(k), z, 0, 128), zm),
        )

    def relay(k):
        shares[k][0].wait_recv()
        a = same(vquarter(chip(k), around(z, -1), 0, 64), zp)
        shares[k][1].wait_recv()
        relays[k] = a, same(vquarter(chip(k), around(z, 1), 64, 64), zm)

    loads[1].wait()
    ka_p = same(kv.at[y, 0, low], yp)
    kb_m = same(kv.at[y, 0, high], ym)
    scores(3)
    v_p.wait_recv()
    share(-1)
    v_m.wait_recv()
    share(1)
    kb_p = same(kv.at[y, 0, high], yp)
    ka_m = same(kv.at[y, 0, low], ym)
    v_f.wait_recv()
    share(2)
    probs(3)
    ka_p.wait_recv()
    k2a = same(kv.at[chip(-1), 0, low], yp)
    kb_m.wait_recv()
    k2b = same(kv.at[chip(1), 0, high], ym)
    relay(-1)
    scores(2, (0,))
    relay(1)
    scores(1, (1,))
    relay(2)
    kb_p.wait_recv()
    scores(2, (1,))
    ka_m.wait_recv()
    scores(1, (0,))
    for k in (-1, 1):
        for r in relays[k]:
            r.wait_recv()
    probs(1)
    probs(2)
    k2a.wait_recv()
    k2b.wait_recv()
    scores(0)
    for r in relays[2]:
        r.wait_recv()
    probs(0)

    stat_pair = send(stat, stat2, partner)
    stat_pair.wait_recv()
    top = jnp.maximum(stat[0:1, :], stat2[0:1, :])
    w1 = jnp.exp2(stat[0:1, :] - top)
    w2 = jnp.exp2(stat2[0:1, :] - top)
    total = stat[1:2, :] * w1 + stat2[1:2, :] * w2
    lse = top + jnp.log2(total)
    gdot = (stat[2:3, :] * w1 + stat2[2:3, :] * w2) / total

    def backward(j):
        out = []
        for half in (0, 1):
            part = pl.ds(half * BLOCK, BLOCK)
            p = jnp.exp2(sc[j, part, :] - lse)
            ds = (p * (dp[j, part, :] - gdot)).astype(BF16)
            dsb[j, part, :] = ds
            out.append((nn(ds, qs[...]), nn(p.astype(BF16), dov[...])))
        return out

    def queries():
        acc = tn(kv[chip(offsets[0]), 0], dsb[0])
        for j in (1, 2, 3):
            acc = acc + tn(kv[chip(offsets[j]), 0], dsb[j])
        return acc

    def up(v):
        return v.astype(F32)

    pieces = [(xp, zi) for xp in range(4) for zi in range(4)]
    place = [lax.rem(zi - z + 5, 4) for zi in range(4)]
    lo, hi = pl.ds(0, 2), pl.ds(2, 2)
    near, far = pl.ds(0, 3), 3
    kc, vc = {}, {}

    def values_second(j):
        vc[j, 1].wait_recv()
        av[j, 2, 0:2] = (up(av[j, 2, 0:2]) + up(rv[0, j])).astype(BF16)
        if j == 0:
            vc[j, 4] = send(av.at[j, 2, lo], dv2.at[0, 0], diag[1, 1])
        else:
            vc[j, 4] = send(av.at[j, 2, lo], fv.at[0, j, lo], zp)
        vc[j, 2].wait_recv()
        av[j, 0, 2:4] = (up(av[j, 0, 2:4]) + up(rv[1, j])).astype(BF16)
        if j == 0:
            vc[j, 6] = send(av.at[j, 0, hi], dv2.at[1, 0], diag[-1, -1])
        else:
            vc[j, 6] = send(av.at[j, 0, hi], fv.at[1, j, hi], zm)

    def values_early():
        vc[0, 5].wait_recv()
        av[0, 1, 0:2] = (up(av[0, 1, 0:2]) + up(fv[1, 0, 0:2])).astype(BF16)
        vc[0, 7] = send(av.at[0, 1, lo], dv2.at[0, 1], yp)
        vc[0, 3].wait_recv()
        av[0, 1, 2:4] = (up(av[0, 1, 2:4]) + up(fv[0, 0, 2:4])).astype(BF16)
        vc[0, 8] = send(av.at[0, 1, hi], dv2.at[1, 1], ym)

    def keys_early():
        kc[5].wait_recv()
        ak[3, 3, 0:2] = (up(ak[3, 3, 0:2]) + up(fk[1, 3, 0:2])).astype(BF16)
        kc[17] = send(ak.at[3, far, lo], dk2.at[0, 1], zp)
        kc[3].wait_recv()
        ak[3, 3, 2:4] = (up(ak[3, 3, 2:4]) + up(fk[0, 3, 2:4])).astype(BF16)
        kc[18] = send(ak.at[3, far, hi], dk2.at[1, 1], zm)

    def block(j):
        for half, (gk_, gv) in enumerate(backward(j)):
            gk_, gv = gk_.astype(BF16), gv.astype(BF16)
            for xp, zi in pieces:
                r0 = (4 * xp + zi) * 32 - half * BLOCK
                if 0 <= r0 < BLOCK:
                    ak[j, place[zi], xp] = gk_[r0 : r0 + 32, :]
                    av[j, place[zi], xp] = gv[r0 : r0 + 32, :]
        for half in (0, 1):
            at_ = (lo, hi)[half]
            to = (zp, zm)[half]
            vc[j, 1 + half] = send(av.at[j, far, at_], rv.at[half, j], to)
            if j == 0:
                kc[1 + half] = send(ak.at[0, pl.ds(0, 4), at_], rk.at[half], (yp, ym)[half])
            if j == 1 and half == 1:
                kc[3] = send(ak.at[1, pl.ds(0, 4), hi], fk.at[0, pl.ds(0, 4), hi], yp)
            if j == 2 and half == 0:
                kc[5] = send(ak.at[2, pl.ds(0, 4), lo], fk.at[1, pl.ds(0, 4), lo], ym)
            if half == 0:
                vc[j, 5] = send(av.at[j, 0, lo], fv.at[1, j, lo], zm)
            else:
                vc[j, 3] = send(av.at[j, 2, hi], fv.at[0, j, hi], zp)

    block(0)
    block(1)
    block(2)
    block(3)
    values_second(0)
    kc[1].wait_recv()
    ak[1, :, 0:2] = (up(ak[1, :, 0:2]) + up(rk[0])).astype(BF16)
    kc[14] = send(ak.at[1, far, lo], dk2.at[0, 0], diag[1, 1])
    kc[4] = send(ak.at[1, near, lo], fk.at[0, pl.ds(0, 3), lo], yp)
    kc[2].wait_recv()
    ak[2, :, 2:4] = (up(ak[2, :, 2:4]) + up(rk[1])).astype(BF16)
    kc[16] = send(ak.at[2, far, hi], dk2.at[1, 0], diag[-1, -1])
    kc[6] = send(ak.at[2, near, hi], fk.at[1, pl.ds(0, 3), hi], ym)
    values_second(1)
    values_early()
    values_second(2)
    values_second(3)

    keys_early()
    dqt[...] = queries()
    dqs[...] = jnp.transpose(dqt[:, theirs])
    dq_pair = send(dqs, dqr, partner)

    def values_along_z(j):
        for i in (3, 4, 5, 6):
            vc[j, i].wait_recv()
        return up(av[j, 1]) + up(fv[0, j]) + up(fv[1, j])

    for i in (4, 6, 7, 8):
        vc[0, i].wait_recv()
    ec = {}
    w = values_along_z(1)
    zv[0, 0:2] = (w[0:2] + up(dv2[0, 0]) + up(dv2[0, 1])).astype(BF16)
    zv[0, 2:4] = w[2:4].astype(BF16)
    ec[0] = send(zv.at[0], fev.at[0], yp)
    w = values_along_z(2)
    zv[1, 0:2] = w[0:2].astype(BF16)
    zv[1, 2:4] = (w[2:4] + up(dv2[1, 0]) + up(dv2[1, 1])).astype(BF16)
    ec[1] = send(zv.at[1], fev.at[1], ym)

    for i in (4, 6):
        kc[i].wait_recv()

    def keys_along_y(q):
        return up(ak[3, q]) + up(fk[0, q]) + up(fk[1, q])

    for i in (14, 16, 17, 18):
        kc[i].wait_recv()
    gc = {}
    w = keys_along_y(2)
    yk[0, 0:2] = (w[0:2] + up(dk2[0, 0]) + up(dk2[0, 1])).astype(BF16)
    yk[0, 2:4] = w[2:4].astype(BF16)
    gc[0] = send(yk.at[0], fgk.at[0], zp)
    w = keys_along_y(0)
    yk[1, 0:2] = w[0:2].astype(BF16)
    yk[1, 2:4] = (w[2:4] + up(dk2[1, 0]) + up(dk2[1, 1])).astype(BF16)
    gc[1] = send(yk.at[1], fgk.at[1], zm)

    w = values_along_z(3)
    for cp in ec.values():
        cp.wait_recv()
    xs[1] = (w + up(fev[0]) + up(fev[1])).astype(BF16)
    xc = []
    for k in (2, 1, 3):
        xc.append(send(xs.at[1, around(x, k)], rx.at[1, x], xo[k - 1]))
    dq_pair.wait_recv()
    dq_out[0] = ((jnp.transpose(dqt[:, mine]) + dqr[...]) * 0.0625).astype(BF16)
    for cp in gc.values():
        cp.wait_recv()
    xs[0] = (keys_along_y(1) + up(fgk[0]) + up(fgk[1])).astype(BF16)
    for k in (2, 1, 3):
        xc.append(send(xs.at[0, around(x, k)], rx.at[0, x], xo[k - 1]))
    rx[0, x] = xs[0, x]
    rx[1, x] = xs[1, x]
    for cp in xc:
        cp.wait_recv()
    for r in (0, 1):
        dk_out[r] = up(rx[0, 2 * r]) + up(rx[0, 2 * r + 1])
        dv_out[r] = up(rx[1, 2 * r]) + up(rx[1, 2 * r + 1])
    for cp in started[-SENDS:]:
        cp.wait_send()
    assert len(started) == COPIES, len(started)


def leave(a, b, c, a_out, b_out, c_out, sem):
    moves = [pltpu.make_async_copy(src, dst, sem.at[i]) for i, (src, dst) in enumerate(((a, a_out), (b, b_out), (c, c_out)))]
    for cp in moves:
        cp.start()
    for cp in moves:
        cp.wait()


def per_device(queries, keys, values, d_out, doc_lengths, fold_order):
    hbm = pl.BlockSpec(memory_space=pl.ANY)
    vmem = pl.BlockSpec(memory_space=pltpu.VMEM)
    smem = pl.BlockSpec(memory_space=pltpu.SMEM)

    def vm(*shape, dtype=BF16):
        return pltpu.VMEM(shape, dtype)

    grads = pl.pallas_call(
        kernel,
        out_shape=(
            pltpu.VMEM((1, 512, 256), BF16),
            pltpu.VMEM((2, 32, 256), F32),
            pltpu.VMEM((2, 32, 256), F32),
        ),
        in_specs=[smem, smem, hbm, hbm, hbm, hbm],
        out_specs=(vmem, vmem, vmem),
        scratch_shapes=[
            vm(1024, 256),
            vm(1024, 256),
            vm(1024, 256),
            vm(256, 1024),
            vm(256, 1024),
            vm(4, 2, 512, 256),
            vm(4, 512, 1024, dtype=F32),
            vm(4, 512, 1024, dtype=F32),
            vm(8, 1024, dtype=F32),
            vm(8, 1024, dtype=F32),
            vm(4, 512, 1024),
            vm(256, 1024, dtype=F32),
            vm(512, 256, dtype=F32),
            vm(512, 256, dtype=F32),
            vm(4, 4, 4, 32, 256),
            vm(4, 4, 4, 32, 256),
            vm(2, 4, 2, 32, 256),
            vm(2, 4, 4, 32, 256),
            vm(2, 2, 2, 32, 256),
            vm(2, 4, 2, 32, 256),
            vm(2, 4, 4, 32, 256),
            vm(2, 2, 2, 32, 256),
            vm(2, 4, 32, 256),
            vm(2, 4, 32, 256),
            vm(2, 4, 32, 256),
            vm(2, 4, 32, 256),
            vm(2, 4, 32, 256),
            vm(2, 4, 32, 256),
            pltpu.SemaphoreType.DMA((4,)),
            pltpu.SemaphoreType.DMA((SENDS,)),
            pltpu.SemaphoreType.DMA((COPIES,)),
        ],
        compiler_params=pltpu.CompilerParams(
            collective_id=0, has_side_effects=True, vmem_limit_bytes=66600000
        ),
    )(doc_lengths, fold_order, queries, keys, values, d_out)
    return pl.pallas_call(
        leave,
        out_shape=tuple(jax.ShapeDtypeStruct(g.shape, g.dtype) for g in grads),
        in_specs=[vmem] * 3,
        out_specs=(hbm,) * 3,
        scratch_shapes=[pltpu.SemaphoreType.DMA((3,))],
        compiler_params=pltpu.CompilerParams(vmem_limit_bytes=1024 * 1024),
    )(*grads)


def solution(mesh):
    in_specs = (
        P("head", "seq", None),
        P(None, "seq", None),
        P(None, "seq", None),
        P("head", "seq", None),
        P(),
        P(),
    )
    out_specs = (
        P("head", "seq", None),
        P(None, ("seq", "head"), None),
        P(None, ("seq", "head"), None),
    )
    return jax.shard_map(
        per_device, mesh=mesh, in_specs=in_specs, out_specs=out_specs, check_vma=False
    )
```

```python
import jax
import jax.numpy as jnp
from jax import lax
from jax.experimental import pallas as pl
from jax.experimental.pallas import tpu as pltpu
from jax.sharding import PartitionSpec as P

MESH = pl.DeviceIdType.MESH
LOG2E = 1.4426950408889634
MASKED = -1e30
BLOCK = 256
F32 = jnp.float32
BF16 = jnp.bfloat16
ROW_HEADS = 8
COPIES = 78
SENDS = 40


def nt(a, b):
    return lax.dot_general(a, b, (((1,), (1,)), ((), ())), preferred_element_type=F32)


def nn(a, b):
    return lax.dot_general(a, b, (((1,), (0,)), ((), ())), preferred_element_type=F32)


def tn(a, b):
    return lax.dot_general(a, b, (((0,), (0,)), ((), ())), preferred_element_type=F32)


def kernel(
    lengths, fold, q_hbm, k_hbm, v_hbm, do_hbm,
    dq_out, dk_out, dv_out,
    qv, dov, qs, qst, dot_, kv, sc, dp, stat, stat2, dsb, dqt, dqs, dqr,
    ak, av, rk, fk, dk2, rv, fv, dv2, zv, fev, yk, fgk, xs, rx,
    local_sem, send_sem, recv_sem,
):
    s = lax.axis_index("seq")
    h = lax.axis_index("head")
    y, c = lax.div(s, 2), lax.rem(s, 2)
    x, z = lax.div(h, 4), lax.rem(h, 4)
    row = lax.div(h, ROW_HEADS)

    def around(v, k):
        return lax.rem(v + (k % 4), 4)

    partner = {"seq": 2 * y + (1 - c), "head": h}
    yp = {"seq": 2 * around(y, 1) + c, "head": h}
    ym = {"seq": 2 * around(y, -1) + c, "head": h}
    yf = {"seq": 2 * around(y, 2) + c, "head": h}
    zp = {"seq": s, "head": 4 * x + around(z, 1)}
    zm = {"seq": s, "head": 4 * x + around(z, -1)}
    diag = {
        (i, j): {"seq": 2 * around(y, i) + c, "head": 4 * x + around(z, j)} for i in (-1, 1) for j in (-1, 1)
    }
    xo = [{"seq": s, "head": 4 * around(x, k) + z} for k in (1, 2, 3)]

    mine = pl.ds(pl.multiple_of(512 * c, 512), 512)
    theirs = pl.ds(pl.multiple_of(512 * (1 - c), 512), 512)

    loads = [
        pltpu.make_async_copy(v_hbm.at[row], kv.at[y, 1], local_sem.at[0]),
        pltpu.make_async_copy(k_hbm.at[row], kv.at[y, 0], local_sem.at[1]),
        pltpu.make_async_copy(q_hbm.at[0], qv.at[mine], local_sem.at[2]),
        pltpu.make_async_copy(do_hbm.at[0], dov.at[mine], local_sem.at[3]),
    ]
    for cp in loads:
        cp.start()

    barrier = pltpu.get_barrier_semaphore()
    peers = [partner, yp, ym, yf, zp, zm] + list(diag.values()) + xo
    for peer in peers:
        pl.semaphore_signal(barrier, inc=1, device_id=peer, device_id_type=MESH)
    pl.semaphore_wait(barrier, len(peers))

    started = []

    def send(src, dst, device):
        i = len(started)
        if i >= SENDS:
            started[i - SENDS].wait_send()
        cp = pltpu.make_async_remote_copy(
            src_ref=src, dst_ref=dst, send_sem=send_sem.at[i % SENDS], recv_sem=recv_sem.at[i],
            device_id=device, device_id_type=MESH,
        )
        cp.start()
        started.append(cp)
        return cp

    def same(ref, device):
        return send(ref, ref, device)

    def chip(k):
        return around(y, k)

    zq = 128 * z

    def vquarter(yi, zi, lo, n):
        return kv.at[yi, 1, pl.ds(pl.multiple_of(128 * zi + lo, 64), n)]

    low, high = pl.ds(0, 128), pl.ds(128, 128)
    xb = lax.rem(x, 2)
    xpair = {"seq": s, "head": 4 * (x + 1 - 2 * xb) + z}

    def khalf(yi, lo, n):
        return kv.at[yi, 0, pl.ds(pl.multiple_of(256 + 128 * xb + lo, 64), n)]

    loads[0].wait()
    v_p = same(vquarter(y, z, 0, 128), yp)
    v_m = same(vquarter(y, z, 0, 128), ym)
    v_f = same(vquarter(y, z, 0, 128), yf)
    loads[2].wait()
    q_pair = same(qv.at[mine], partner)
    loads[3].wait()
    do_pair = same(dov.at[mine], partner)

    lane = lax.broadcasted_iota(jnp.int32, (1, 1024), 1)
    pos = lane + fold[4 * y] * BLOCK
    for b in (1, 2, 3):
        pos = jnp.where(lane < BLOCK * b, pos, lane + (fold[4 * y + b] - b) * BLOCK)
    first = jnp.zeros((1, 1024), jnp.int32)
    at = jnp.int32(0)
    for d in range(8):
        first = jnp.where(pos >= at, at, first)
        at = at + lengths[row, d]
    rows = lax.broadcasted_iota(jnp.int32, (BLOCK, 1024), 0)
    stat[0:1, :] = jnp.full((1, 1024), MASKED, F32)
    stat[1:3, :] = jnp.zeros((2, 1024), F32)
    stat[3:4, :] = jnp.full((1, 1024), MASKED, F32)
    stat[4:8, :] = jnp.zeros((4, 1024), F32)
    q_pair.wait_recv()
    qs[...] = (qv[...].astype(F32) * 0.0625).astype(BF16)
    qst[...] = jnp.transpose(qs[...])
    do_pair.wait_recv()
    dot_[...] = jnp.transpose(dov[...])

    offsets = (2, 1, -1, 0)

    parts = [pl.ds(half * BLOCK, BLOCK) for half in (0, 1)]

    def scores(j, halves=(0, 1)):
        yi = chip(offsets[j])
        m = stat[0:1, :]
        for half in halves:
            part = parts[half]
            base = fold[4 * yi + 2 * c + half] * BLOCK
            raw = nn(kv[yi, 0, part, :], qst[...])
            ok = (rows >= first - base) & (rows <= pos - base)
            s2 = jnp.where(ok, raw * LOG2E, MASKED)
            sc[j, part, :] = s2
            m = jnp.maximum(m, jnp.max(s2, axis=0, keepdims=True))
        stat[0:1, :] = m

    def probs(j):
        yi = chip(offsets[j])
        m = stat[0:1, :]
        alpha = jnp.exp2(stat[3:4, :] - m)
        total = stat[1:2, :] * alpha
        dot = stat[2:3, :] * alpha
        for part in parts:
            gp = nn(kv[yi, 1, part, :], dot_[...])
            dp[j, part, :] = gp
            e = jnp.exp2(sc[j, part, :] - m)
            total = total + jnp.sum(e, axis=0, keepdims=True)
            dot = dot + jnp.sum(e * gp, axis=0, keepdims=True)
        stat[1:2, :] = total
        stat[2:3, :] = dot
        stat[3:4, :] = m

    shares, relays = {}, {}

    def share(k):
        shares[k] = (
            same(vquarter(chip(k), z, 0, 128), zp),
            same(vquarter(chip(k), z, 0, 128), zm),
        )

    def relay(k):
        shares[k][0].wait_recv()
        a = same(vquarter(chip(k), around(z, -1), 0, 64), zp)
        shares[k][1].wait_recv()
        relays[k] = a, same(vquarter(chip(k), around(z, 1), 64, 64), zm)

    loads[1].wait()
    kx_p = same(khalf(y, 0, 128), yp)
    kx_m = same(khalf(y, 0, 128), ym)
    ka_p = same(kv.at[y, 0, low], yp)
    kb_m = same(kv.at[y, 0, high], ym)
    scores(3)
    v_p.wait_recv()
    share(-1)
    v_m.wait_recv()
    share(1)
    kb_p = same(kv.at[y, 0, high], yp)
    ka_m = same(kv.at[y, 0, low], ym)
    v_f.wait_recv()
    share(2)
    probs(3)
    cross = {}
    kx_p.wait_recv()
    x2a = same(khalf(chip(-1), 0, 64), yp)
    cross[-1] = same(khalf(chip(-1), 0, 128), xpair)
    kx_m.wait_recv()
    x2b = same(khalf(chip(1), 64, 64), ym)
    cross[1] = same(khalf(chip(1), 0, 128), xpair)
    ka_p.wait_recv()
    k2a = same(kv.at[chip(-1), 0, low], yp)
    kb_m.wait_recv()
    k2b = same(kv.at[chip(1), 0, high], ym)
    relay(-1)
    relay(1)
    kb_p.wait_recv()
    scores(2, (0,))
    x2a.wait_recv()
    x2b.wait_recv()
    cross[2] = same(khalf(chip(2), 0, 128), xpair)
    relay(2)
    ka_m.wait_recv()
    scores(1, (0,))
    cross[-1].wait_recv()
    scores(2, (1,))
    cross[1].wait_recv()
    scores(1, (1,))
    k2a.wait_recv()
    k2b.wait_recv()
    scores(0, (0,))
    for k in (-1, 1):
        for r in relays[k]:
            r.wait_recv()
    probs(1)
    probs(2)
    cross[2].wait_recv()
    scores(0, (1,))
    for r in relays[2]:
        r.wait_recv()
    probs(0)

    stat_pair = send(stat, stat2, partner)
    stat_pair.wait_recv()
    top = jnp.maximum(stat[0:1, :], stat2[0:1, :])
    w1 = jnp.exp2(stat[0:1, :] - top)
    w2 = jnp.exp2(stat2[0:1, :] - top)
    total = stat[1:2, :] * w1 + stat2[1:2, :] * w2
    lse = top + jnp.log2(total)
    gdot = (stat[2:3, :] * w1 + stat2[2:3, :] * w2) / total

    def backward(j):
        out = []
        for half in (0, 1):
            part = pl.ds(half * BLOCK, BLOCK)
            p = jnp.exp2(sc[j, part, :] - lse)
            ds = (p * (dp[j, part, :] - gdot)).astype(BF16)
            dsb[j, part, :] = ds
            out.append((nn(ds, qs[...]), nn(p.astype(BF16), dov[...])))
        return out

    def queries():
        acc = tn(kv[chip(offsets[0]), 0], dsb[0])
        for j in (1, 2, 3):
            acc = acc + tn(kv[chip(offsets[j]), 0], dsb[j])
        return acc

    def up(v):
        return v.astype(F32)

    pieces = [(xp, zi) for xp in range(4) for zi in range(4)]
    place = [lax.rem(zi - z + 5, 4) for zi in range(4)]
    lo, hi = pl.ds(0, 2), pl.ds(2, 2)
    near, far = pl.ds(0, 3), 3
    kc, vc = {}, {}

    def values_second(j):
        vc[j, 1].wait_recv()
        av[j, 2, 0:2] = (up(av[j, 2, 0:2]) + up(rv[0, j])).astype(BF16)
        if j == 0:
            vc[j, 4] = send(av.at[j, 2, lo], dv2.at[0, 0], diag[1, 1])
        else:
            vc[j, 4] = send(av.at[j, 2, lo], fv.at[0, j, lo], zp)
        vc[j, 2].wait_recv()
        av[j, 0, 2:4] = (up(av[j, 0, 2:4]) + up(rv[1, j])).astype(BF16)
        if j == 0:
            vc[j, 6] = send(av.at[j, 0, hi], dv2.at[1, 0], diag[-1, -1])
        else:
            vc[j, 6] = send(av.at[j, 0, hi], fv.at[1, j, hi], zm)

    def values_early():
        vc[0, 5].wait_recv()
        av[0, 1, 0:2] = (up(av[0, 1, 0:2]) + up(fv[1, 0, 0:2])).astype(BF16)
        vc[0, 7] = send(av.at[0, 1, lo], dv2.at[0, 1], yp)
        vc[0, 3].wait_recv()
        av[0, 1, 2:4] = (up(av[0, 1, 2:4]) + up(fv[0, 0, 2:4])).astype(BF16)
        vc[0, 8] = send(av.at[0, 1, hi], dv2.at[1, 1], ym)

    def keys_early():
        kc[5].wait_recv()
        ak[3, 3, 0:2] = (up(ak[3, 3, 0:2]) + up(fk[1, 3, 0:2])).astype(BF16)
        kc[17] = send(ak.at[3, far, lo], dk2.at[0, 1], zp)
        kc[3].wait_recv()
        ak[3, 3, 2:4] = (up(ak[3, 3, 2:4]) + up(fk[0, 3, 2:4])).astype(BF16)
        kc[18] = send(ak.at[3, far, hi], dk2.at[1, 1], zm)

    def block(j):
        for half, (gk_, gv) in enumerate(backward(j)):
            gk_, gv = gk_.astype(BF16), gv.astype(BF16)
            for xp, zi in pieces:
                r0 = (4 * xp + zi) * 32 - half * BLOCK
                if 0 <= r0 < BLOCK:
                    ak[j, place[zi], xp] = gk_[r0 : r0 + 32, :]
                    av[j, place[zi], xp] = gv[r0 : r0 + 32, :]
        for half in (0, 1):
            at_ = (lo, hi)[half]
            to = (zp, zm)[half]
            vc[j, 1 + half] = send(av.at[j, far, at_], rv.at[half, j], to)
            if j == 0:
                kc[1 + half] = send(ak.at[0, pl.ds(0, 4), at_], rk.at[half], (yp, ym)[half])
            if j == 1 and half == 1:
                kc[3] = send(ak.at[1, pl.ds(0, 4), hi], fk.at[0, pl.ds(0, 4), hi], yp)
            if j == 2 and half == 0:
                kc[5] = send(ak.at[2, pl.ds(0, 4), lo], fk.at[1, pl.ds(0, 4), lo], ym)
            if half == 0:
                vc[j, 5] = send(av.at[j, 0, lo], fv.at[1, j, lo], zm)
            else:
                vc[j, 3] = send(av.at[j, 2, hi], fv.at[0, j, hi], zp)

    block(0)
    block(1)
    block(2)
    block(3)
    values_second(0)
    kc[1].wait_recv()
    ak[1, :, 0:2] = (up(ak[1, :, 0:2]) + up(rk[0])).astype(BF16)
    kc[14] = send(ak.at[1, far, lo], dk2.at[0, 0], diag[1, 1])
    kc[4] = send(ak.at[1, near, lo], fk.at[0, pl.ds(0, 3), lo], yp)
    kc[2].wait_recv()
    ak[2, :, 2:4] = (up(ak[2, :, 2:4]) + up(rk[1])).astype(BF16)
    kc[16] = send(ak.at[2, far, hi], dk2.at[1, 0], diag[-1, -1])
    kc[6] = send(ak.at[2, near, hi], fk.at[1, pl.ds(0, 3), hi], ym)
    values_second(1)
    values_early()
    values_second(2)
    values_second(3)

    keys_early()
    dqt[...] = queries()
    dqs[...] = jnp.transpose(dqt[:, theirs])
    dq_pair = send(dqs, dqr, partner)

    def values_along_z(j):
        for i in (3, 4, 5, 6):
            vc[j, i].wait_recv()
        return up(av[j, 1]) + up(fv[0, j]) + up(fv[1, j])

    for i in (4, 6, 7, 8):
        vc[0, i].wait_recv()
    ec = {}
    w = values_along_z(1)
    zv[0, 0:2] = (w[0:2] + up(dv2[0, 0]) + up(dv2[0, 1])).astype(BF16)
    zv[0, 2:4] = w[2:4].astype(BF16)
    ec[0] = send(zv.at[0], fev.at[0], yp)
    w = values_along_z(2)
    zv[1, 0:2] = w[0:2].astype(BF16)
    zv[1, 2:4] = (w[2:4] + up(dv2[1, 0]) + up(dv2[1, 1])).astype(BF16)
    ec[1] = send(zv.at[1], fev.at[1], ym)

    for i in (4, 6):
        kc[i].wait_recv()

    def keys_along_y(q):
        return up(ak[3, q]) + up(fk[0, q]) + up(fk[1, q])

    for i in (14, 16, 17, 18):
        kc[i].wait_recv()
    gc = {}
    w = keys_along_y(2)
    yk[0, 0:2] = (w[0:2] + up(dk2[0, 0]) + up(dk2[0, 1])).astype(BF16)
    yk[0, 2:4] = w[2:4].astype(BF16)
    gc[0] = send(yk.at[0], fgk.at[0], zp)
    w = keys_along_y(0)
    yk[1, 0:2] = w[0:2].astype(BF16)
    yk[1, 2:4] = (w[2:4] + up(dk2[1, 0]) + up(dk2[1, 1])).astype(BF16)
    gc[1] = send(yk.at[1], fgk.at[1], zm)

    w = values_along_z(3)
    for cp in ec.values():
        cp.wait_recv()
    xs[1] = (w + up(fev[0]) + up(fev[1])).astype(BF16)
    xc = []
    for k in (2, 1, 3):
        xc.append(send(xs.at[1, around(x, k)], rx.at[1, x], xo[k - 1]))
    dq_pair.wait_recv()
    dq_out[0] = ((jnp.transpose(dqt[:, mine]) + dqr[...]) * 0.0625).astype(BF16)
    for cp in gc.values():
        cp.wait_recv()
    xs[0] = (keys_along_y(1) + up(fgk[0]) + up(fgk[1])).astype(BF16)
    for k in (2, 1, 3):
        xc.append(send(xs.at[0, around(x, k)], rx.at[0, x], xo[k - 1]))
    rx[0, x] = xs[0, x]
    rx[1, x] = xs[1, x]
    for cp in xc:
        cp.wait_recv()
    for r in (0, 1):
        dk_out[r] = up(rx[0, 2 * r]) + up(rx[0, 2 * r + 1])
        dv_out[r] = up(rx[1, 2 * r]) + up(rx[1, 2 * r + 1])
    for cp in started[-SENDS:]:
        cp.wait_send()
    assert len(started) == COPIES, len(started)


def leave(a, b, c, a_out, b_out, c_out, sem):
    moves = [pltpu.make_async_copy(src, dst, sem.at[i]) for i, (src, dst) in enumerate(((a, a_out), (b, b_out), (c, c_out)))]
    for cp in moves:
        cp.start()
    for cp in moves:
        cp.wait()


def per_device(queries, keys, values, d_out, doc_lengths, fold_order):
    hbm = pl.BlockSpec(memory_space=pl.ANY)
    vmem = pl.BlockSpec(memory_space=pltpu.VMEM)
    smem = pl.BlockSpec(memory_space=pltpu.SMEM)

    def vm(*shape, dtype=BF16):
        return pltpu.VMEM(shape, dtype)

    grads = pl.pallas_call(
        kernel,
        out_shape=(
            pltpu.VMEM((1, 512, 256), BF16),
            pltpu.VMEM((2, 32, 256), F32),
            pltpu.VMEM((2, 32, 256), F32),
        ),
        in_specs=[smem, smem, hbm, hbm, hbm, hbm],
        out_specs=(vmem, vmem, vmem),
        scratch_shapes=[
            vm(1024, 256),
            vm(1024, 256),
            vm(1024, 256),
            vm(256, 1024),
            vm(256, 1024),
            vm(4, 2, 512, 256),
            vm(4, 512, 1024, dtype=F32),
            vm(4, 512, 1024, dtype=F32),
            vm(8, 1024, dtype=F32),
            vm(8, 1024, dtype=F32),
            vm(4, 512, 1024),
            vm(256, 1024, dtype=F32),
            vm(512, 256, dtype=F32),
            vm(512, 256, dtype=F32),
            vm(4, 4, 4, 32, 256),
            vm(4, 4, 4, 32, 256),
            vm(2, 4, 2, 32, 256),
            vm(2, 4, 4, 32, 256),
            vm(2, 2, 2, 32, 256),
            vm(2, 4, 2, 32, 256),
            vm(2, 4, 4, 32, 256),
            vm(2, 2, 2, 32, 256),
            vm(2, 4, 32, 256),
            vm(2, 4, 32, 256),
            vm(2, 4, 32, 256),
            vm(2, 4, 32, 256),
            vm(2, 4, 32, 256),
            vm(2, 4, 32, 256),
            pltpu.SemaphoreType.DMA((4,)),
            pltpu.SemaphoreType.DMA((SENDS,)),
            pltpu.SemaphoreType.DMA((COPIES,)),
        ],
        compiler_params=pltpu.CompilerParams(
            collective_id=0, has_side_effects=True, vmem_limit_bytes=66600000
        ),
    )(doc_lengths, fold_order, queries, keys, values, d_out)
    return pl.pallas_call(
        leave,
        out_shape=tuple(jax.ShapeDtypeStruct(g.shape, g.dtype) for g in grads),
        in_specs=[vmem] * 3,
        out_specs=(hbm,) * 3,
        scratch_shapes=[pltpu.SemaphoreType.DMA((3,))],
        compiler_params=pltpu.CompilerParams(vmem_limit_bytes=1024 * 1024),
    )(*grads)


def solution(mesh):
    in_specs = (
        P("head", "seq", None),
        P(None, "seq", None),
        P(None, "seq", None),
        P("head", "seq", None),
        P(),
        P(),
    )
    out_specs = (
        P("head", "seq", None),
        P(None, ("seq", "head"), None),
        P(None, ("seq", "head"), None),
    )
    return jax.shard_map(
        per_device, mesh=mesh, in_specs=in_specs, out_specs=out_specs, check_vma=False
    )
```

```python
import jax
import jax.numpy as jnp
from jax import lax
from jax.experimental import pallas as pl
from jax.experimental.pallas import tpu as pltpu
from jax.sharding import PartitionSpec as P

MESH = pl.DeviceIdType.MESH
LOG2E = 1.4426950408889634
MASKED = -1e30
BLOCK = 256
F32 = jnp.float32
BF16 = jnp.bfloat16
ROW_HEADS = 8
COPIES = 78
SENDS = 40


def nt(a, b):
    return lax.dot_general(a, b, (((1,), (1,)), ((), ())), preferred_element_type=F32)


def nn(a, b):
    return lax.dot_general(a, b, (((1,), (0,)), ((), ())), preferred_element_type=F32)


def tn(a, b):
    return lax.dot_general(a, b, (((0,), (0,)), ((), ())), preferred_element_type=F32)


def kernel(
    lengths, fold, q_hbm, k_hbm, v_hbm, do_hbm,
    dq_out, dk_out, dv_out,
    qv, dov, qs, qst, dot_, kv, sc, dp, stat, stat2, dsb, dqt, dqs, dqr,
    ak, av, rk, fk, dk2, rv, fv, dv2, zv, fev, yk, fgk, xs, rx,
    local_sem, send_sem, recv_sem,
):
    s = lax.axis_index("seq")
    h = lax.axis_index("head")
    y, c = lax.div(s, 2), lax.rem(s, 2)
    x, z = lax.div(h, 4), lax.rem(h, 4)
    row = lax.div(h, ROW_HEADS)

    def around(v, k):
        return lax.rem(v + (k % 4), 4)

    partner = {"seq": 2 * y + (1 - c), "head": h}
    yp = {"seq": 2 * around(y, 1) + c, "head": h}
    ym = {"seq": 2 * around(y, -1) + c, "head": h}
    yf = {"seq": 2 * around(y, 2) + c, "head": h}
    zp = {"seq": s, "head": 4 * x + around(z, 1)}
    zm = {"seq": s, "head": 4 * x + around(z, -1)}
    diag = {
        (i, j): {"seq": 2 * around(y, i) + c, "head": 4 * x + around(z, j)} for i in (-1, 1) for j in (-1, 1)
    }
    xo = [{"seq": s, "head": 4 * around(x, k) + z} for k in (1, 2, 3)]

    mine = pl.ds(pl.multiple_of(512 * c, 512), 512)
    theirs = pl.ds(pl.multiple_of(512 * (1 - c), 512), 512)

    loads = [
        pltpu.make_async_copy(v_hbm.at[row], kv.at[y, 1], local_sem.at[0]),
        pltpu.make_async_copy(k_hbm.at[row], kv.at[y, 0], local_sem.at[1]),
        pltpu.make_async_copy(q_hbm.at[0], qv.at[mine], local_sem.at[2]),
        pltpu.make_async_copy(do_hbm.at[0], dov.at[mine], local_sem.at[3]),
    ]
    for cp in loads:
        cp.start()

    barrier = pltpu.get_barrier_semaphore()
    peers = [partner, yp, ym, yf, zp, zm] + list(diag.values()) + xo
    for peer in peers:
        pl.semaphore_signal(barrier, inc=1, device_id=peer, device_id_type=MESH)
    pl.semaphore_wait(barrier, len(peers))

    started = []

    def send(src, dst, device):
        i = len(started)
        if i >= SENDS:
            started[i - SENDS].wait_send()
        cp = pltpu.make_async_remote_copy(
            src_ref=src, dst_ref=dst, send_sem=send_sem.at[i % SENDS], recv_sem=recv_sem.at[i],
            device_id=device, device_id_type=MESH,
        )
        cp.start()
        started.append(cp)
        return cp

    def same(ref, device):
        return send(ref, ref, device)

    def chip(k):
        return around(y, k)

    zq = 128 * z

    def vquarter(yi, zi, lo, n):
        return kv.at[yi, 1, pl.ds(pl.multiple_of(128 * zi + lo, 64), n)]

    low, high = pl.ds(0, 128), pl.ds(128, 128)
    xb = lax.rem(x, 2)
    xpair = {"seq": s, "head": 4 * (x + 1 - 2 * xb) + z}

    def khalf(yi, lo, n):
        return kv.at[yi, 0, pl.ds(pl.multiple_of(256 + 128 * xb + lo, 64), n)]

    loads[0].wait()
    v_p = same(vquarter(y, z, 0, 128), yp)
    v_m = same(vquarter(y, z, 0, 128), ym)
    v_f = same(vquarter(y, z, 0, 128), yf)
    loads[2].wait()
    q_pair = same(qv.at[mine], partner)
    loads[3].wait()
    do_pair = same(dov.at[mine], partner)

    lane = lax.broadcasted_iota(jnp.int32, (1, 1024), 1)
    pos = lane + fold[4 * y] * BLOCK
    for b in (1, 2, 3):
        pos = jnp.where(lane < BLOCK * b, pos, lane + (fold[4 * y + b] - b) * BLOCK)
    first = jnp.zeros((1, 1024), jnp.int32)
    at = jnp.int32(0)
    for d in range(8):
        first = jnp.where(pos >= at, at, first)
        at = at + lengths[row, d]
    rows = lax.broadcasted_iota(jnp.int32, (BLOCK, 1024), 0)
    stat[0:1, :] = jnp.full((1, 1024), MASKED, F32)
    stat[1:3, :] = jnp.zeros((2, 1024), F32)
    stat[3:4, :] = jnp.full((1, 1024), MASKED, F32)
    stat[4:8, :] = jnp.zeros((4, 1024), F32)
    q_pair.wait_recv()
    qs[...] = (qv[...].astype(F32) * 0.0625).astype(BF16)
    qst[...] = jnp.transpose(qs[...])
    do_pair.wait_recv()
    dot_[...] = jnp.transpose(dov[...])

    offsets = (2, 1, -1, 0)

    parts = [pl.ds(half * BLOCK, BLOCK) for half in (0, 1)]

    def scores(j, half, off=0, n=BLOCK):
        yi = chip(offsets[j])
        part = pl.ds(pl.multiple_of(half * BLOCK + off, 128), n)
        base = fold[4 * yi + 2 * c + half] * BLOCK + off
        raw = nn(kv[yi, 0, part, :], qst[...])
        ok = (rows[:n] >= first - base) & (rows[:n] <= pos - base)
        s2 = jnp.where(ok, raw * LOG2E, MASKED)
        sc[j, part, :] = s2
        stat[0:1, :] = jnp.maximum(stat[0:1, :], jnp.max(s2, axis=0, keepdims=True))

    def probs(j):
        yi = chip(offsets[j])
        m = stat[0:1, :]
        alpha = jnp.exp2(stat[3:4, :] - m)
        total = stat[1:2, :] * alpha
        dot = stat[2:3, :] * alpha
        for part in parts:
            gp = nn(kv[yi, 1, part, :], dot_[...])
            dp[j, part, :] = gp
            e = jnp.exp2(sc[j, part, :] - m)
            total = total + jnp.sum(e, axis=0, keepdims=True)
            dot = dot + jnp.sum(e * gp, axis=0, keepdims=True)
        stat[1:2, :] = total
        stat[2:3, :] = dot
        stat[3:4, :] = m

    shares, relays = {}, {}

    def share(k):
        shares[k] = (
            same(vquarter(chip(k), z, 0, 128), zp),
            same(vquarter(chip(k), z, 0, 128), zm),
        )

    def relay(k):
        shares[k][0].wait_recv()
        a = same(vquarter(chip(k), around(z, -1), 0, 64), zp)
        shares[k][1].wait_recv()
        relays[k] = a, same(vquarter(chip(k), around(z, 1), 64, 64), zm)

    loads[1].wait()
    kx_p = same(khalf(y, 0, 128), yp)
    kx_m = same(khalf(y, 0, 128), ym)
    ka_p = same(kv.at[y, 0, low], yp)
    kb_m = same(kv.at[y, 0, high], ym)
    scores(3, 0)
    scores(3, 1)
    v_p.wait_recv()
    share(-1)
    v_m.wait_recv()
    share(1)
    kb_p = same(kv.at[y, 0, high], yp)
    ka_m = same(kv.at[y, 0, low], ym)
    v_f.wait_recv()
    share(2)
    probs(3)
    cross = {}
    kx_p.wait_recv()
    x2a = same(khalf(chip(-1), 0, 64), yp)
    cross[-1] = same(khalf(chip(-1), 0, 128), xpair)
    kx_m.wait_recv()
    x2b = same(khalf(chip(1), 64, 64), ym)
    cross[1] = same(khalf(chip(1), 0, 128), xpair)
    scores(2, 1, 128 * xb, 128)
    scores(1, 1, 128 * xb, 128)
    ka_p.wait_recv()
    k2a = same(kv.at[chip(-1), 0, low], yp)
    kb_m.wait_recv()
    k2b = same(kv.at[chip(1), 0, high], ym)
    scores(2, 0, 0, 128)
    relay(-1)
    scores(1, 0, 128, 128)
    relay(1)
    kb_p.wait_recv()
    scores(2, 0, 128, 128)
    x2a.wait_recv()
    x2b.wait_recv()
    cross[2] = same(khalf(chip(2), 0, 128), xpair)
    relay(2)
    ka_m.wait_recv()
    scores(1, 0, 0, 128)
    cross[-1].wait_recv()
    scores(2, 1, 128 * (1 - xb), 128)
    cross[1].wait_recv()
    scores(1, 1, 128 * (1 - xb), 128)
    k2a.wait_recv()
    k2b.wait_recv()
    scores(0, 0)
    for r in relays[-1]:
        r.wait_recv()
    probs(2)
    for r in relays[1]:
        r.wait_recv()
    probs(1)
    cross[2].wait_recv()
    scores(0, 1)
    for r in relays[2]:
        r.wait_recv()
    probs(0)

    stat_pair = send(stat, stat2, partner)
    stat_pair.wait_recv()
    top = jnp.maximum(stat[0:1, :], stat2[0:1, :])
    w1 = jnp.exp2(stat[0:1, :] - top)
    w2 = jnp.exp2(stat2[0:1, :] - top)
    total = stat[1:2, :] * w1 + stat2[1:2, :] * w2
    lse = top + jnp.log2(total)
    gdot = (stat[2:3, :] * w1 + stat2[2:3, :] * w2) / total

    def backward(j):
        out = []
        for half in (0, 1):
            part = pl.ds(half * BLOCK, BLOCK)
            p = jnp.exp2(sc[j, part, :] - lse)
            ds = (p * (dp[j, part, :] - gdot)).astype(BF16)
            dsb[j, part, :] = ds
            out.append((nn(ds, qs[...]), nn(p.astype(BF16), dov[...])))
        return out

    def queries():
        acc = tn(kv[chip(offsets[0]), 0], dsb[0])
        for j in (1, 2, 3):
            acc = acc + tn(kv[chip(offsets[j]), 0], dsb[j])
        return acc

    def up(v):
        return v.astype(F32)

    pieces = [(xp, zi) for xp in range(4) for zi in range(4)]
    place = [lax.rem(zi - z + 5, 4) for zi in range(4)]
    lo, hi = pl.ds(0, 2), pl.ds(2, 2)
    near, far = pl.ds(0, 3), 3
    kc, vc = {}, {}

    def values_second(j):
        vc[j, 1].wait_recv()
        av[j, 2, 0:2] = (up(av[j, 2, 0:2]) + up(rv[0, j])).astype(BF16)
        if j == 0:
            vc[j, 4] = send(av.at[j, 2, lo], dv2.at[0, 0], diag[1, 1])
        else:
            vc[j, 4] = send(av.at[j, 2, lo], fv.at[0, j, lo], zp)
        vc[j, 2].wait_recv()
        av[j, 0, 2:4] = (up(av[j, 0, 2:4]) + up(rv[1, j])).astype(BF16)
        if j == 0:
            vc[j, 6] = send(av.at[j, 0, hi], dv2.at[1, 0], diag[-1, -1])
        else:
            vc[j, 6] = send(av.at[j, 0, hi], fv.at[1, j, hi], zm)

    def values_early():
        vc[0, 5].wait_recv()
        av[0, 1, 0:2] = (up(av[0, 1, 0:2]) + up(fv[1, 0, 0:2])).astype(BF16)
        vc[0, 7] = send(av.at[0, 1, lo], dv2.at[0, 1], yp)
        vc[0, 3].wait_recv()
        av[0, 1, 2:4] = (up(av[0, 1, 2:4]) + up(fv[0, 0, 2:4])).astype(BF16)
        vc[0, 8] = send(av.at[0, 1, hi], dv2.at[1, 1], ym)

    def keys_early():
        kc[5].wait_recv()
        ak[3, 3, 0:2] = (up(ak[3, 3, 0:2]) + up(fk[1, 3, 0:2])).astype(BF16)
        kc[17] = send(ak.at[3, far, lo], dk2.at[0, 1], zp)
        kc[3].wait_recv()
        ak[3, 3, 2:4] = (up(ak[3, 3, 2:4]) + up(fk[0, 3, 2:4])).astype(BF16)
        kc[18] = send(ak.at[3, far, hi], dk2.at[1, 1], zm)

    def block(j):
        for half, (gk_, gv) in enumerate(backward(j)):
            gk_, gv = gk_.astype(BF16), gv.astype(BF16)
            for xp, zi in pieces:
                r0 = (4 * xp + zi) * 32 - half * BLOCK
                if 0 <= r0 < BLOCK:
                    ak[j, place[zi], xp] = gk_[r0 : r0 + 32, :]
                    av[j, place[zi], xp] = gv[r0 : r0 + 32, :]
        for half in (0, 1):
            at_ = (lo, hi)[half]
            to = (zp, zm)[half]
            vc[j, 1 + half] = send(av.at[j, far, at_], rv.at[half, j], to)
            if j == 0:
                kc[1 + half] = send(ak.at[0, pl.ds(0, 4), at_], rk.at[half], (yp, ym)[half])
            if j == 1 and half == 1:
                kc[3] = send(ak.at[1, pl.ds(0, 4), hi], fk.at[0, pl.ds(0, 4), hi], yp)
            if j == 2 and half == 0:
                kc[5] = send(ak.at[2, pl.ds(0, 4), lo], fk.at[1, pl.ds(0, 4), lo], ym)
            if half == 0:
                vc[j, 5] = send(av.at[j, 0, lo], fv.at[1, j, lo], zm)
            else:
                vc[j, 3] = send(av.at[j, 2, hi], fv.at[0, j, hi], zp)

    block(0)
    block(1)
    block(2)
    block(3)
    values_second(0)
    kc[1].wait_recv()
    ak[1, :, 0:2] = (up(ak[1, :, 0:2]) + up(rk[0])).astype(BF16)
    kc[14] = send(ak.at[1, far, lo], dk2.at[0, 0], diag[1, 1])
    kc[4] = send(ak.at[1, near, lo], fk.at[0, pl.ds(0, 3), lo], yp)
    kc[2].wait_recv()
    ak[2, :, 2:4] = (up(ak[2, :, 2:4]) + up(rk[1])).astype(BF16)
    kc[16] = send(ak.at[2, far, hi], dk2.at[1, 0], diag[-1, -1])
    kc[6] = send(ak.at[2, near, hi], fk.at[1, pl.ds(0, 3), hi], ym)
    values_second(1)
    values_early()
    values_second(2)
    values_second(3)

    keys_early()
    dqt[...] = queries()
    dqs[...] = jnp.transpose(dqt[:, theirs])
    dq_pair = send(dqs, dqr, partner)

    def values_along_z(j):
        for i in (3, 4, 5, 6):
            vc[j, i].wait_recv()
        return up(av[j, 1]) + up(fv[0, j]) + up(fv[1, j])

    for i in (4, 6, 7, 8):
        vc[0, i].wait_recv()
    ec = {}
    w = values_along_z(1)
    zv[0, 0:2] = (w[0:2] + up(dv2[0, 0]) + up(dv2[0, 1])).astype(BF16)
    zv[0, 2:4] = w[2:4].astype(BF16)
    ec[0] = send(zv.at[0], fev.at[0], yp)
    w = values_along_z(2)
    zv[1, 0:2] = w[0:2].astype(BF16)
    zv[1, 2:4] = (w[2:4] + up(dv2[1, 0]) + up(dv2[1, 1])).astype(BF16)
    ec[1] = send(zv.at[1], fev.at[1], ym)

    for i in (4, 6):
        kc[i].wait_recv()

    def keys_along_y(q):
        return up(ak[3, q]) + up(fk[0, q]) + up(fk[1, q])

    for i in (14, 16, 17, 18):
        kc[i].wait_recv()
    gc = {}
    w = keys_along_y(2)
    yk[0, 0:2] = (w[0:2] + up(dk2[0, 0]) + up(dk2[0, 1])).astype(BF16)
    yk[0, 2:4] = w[2:4].astype(BF16)
    gc[0] = send(yk.at[0], fgk.at[0], zp)
    w = keys_along_y(0)
    yk[1, 0:2] = w[0:2].astype(BF16)
    yk[1, 2:4] = (w[2:4] + up(dk2[1, 0]) + up(dk2[1, 1])).astype(BF16)
    gc[1] = send(yk.at[1], fgk.at[1], zm)

    w = values_along_z(3)
    for cp in ec.values():
        cp.wait_recv()
    xs[1] = (w + up(fev[0]) + up(fev[1])).astype(BF16)
    xc = []
    for k in (2, 1, 3):
        xc.append(send(xs.at[1, around(x, k)], rx.at[1, x], xo[k - 1]))
    dq_pair.wait_recv()
    dq_out[0] = ((jnp.transpose(dqt[:, mine]) + dqr[...]) * 0.0625).astype(BF16)
    for cp in gc.values():
        cp.wait_recv()
    xs[0] = (keys_along_y(1) + up(fgk[0]) + up(fgk[1])).astype(BF16)
    for k in (2, 1, 3):
        xc.append(send(xs.at[0, around(x, k)], rx.at[0, x], xo[k - 1]))
    rx[0, x] = xs[0, x]
    rx[1, x] = xs[1, x]
    for cp in xc:
        cp.wait_recv()
    for r in (0, 1):
        dk_out[r] = up(rx[0, 2 * r]) + up(rx[0, 2 * r + 1])
        dv_out[r] = up(rx[1, 2 * r]) + up(rx[1, 2 * r + 1])
    for cp in started[-SENDS:]:
        cp.wait_send()
    assert len(started) == COPIES, len(started)


def leave(a, b, c, a_out, b_out, c_out, sem):
    moves = [pltpu.make_async_copy(src, dst, sem.at[i]) for i, (src, dst) in enumerate(((a, a_out), (b, b_out), (c, c_out)))]
    for cp in moves:
        cp.start()
    for cp in moves:
        cp.wait()


def per_device(queries, keys, values, d_out, doc_lengths, fold_order):
    hbm = pl.BlockSpec(memory_space=pl.ANY)
    vmem = pl.BlockSpec(memory_space=pltpu.VMEM)
    smem = pl.BlockSpec(memory_space=pltpu.SMEM)

    def vm(*shape, dtype=BF16):
        return pltpu.VMEM(shape, dtype)

    grads = pl.pallas_call(
        kernel,
        out_shape=(
            pltpu.VMEM((1, 512, 256), BF16),
            pltpu.VMEM((2, 32, 256), F32),
            pltpu.VMEM((2, 32, 256), F32),
        ),
        in_specs=[smem, smem, hbm, hbm, hbm, hbm],
        out_specs=(vmem, vmem, vmem),
        scratch_shapes=[
            vm(1024, 256),
            vm(1024, 256),
            vm(1024, 256),
            vm(256, 1024),
            vm(256, 1024),
            vm(4, 2, 512, 256),
            vm(4, 512, 1024, dtype=F32),
            vm(4, 512, 1024, dtype=F32),
            vm(8, 1024, dtype=F32),
            vm(8, 1024, dtype=F32),
            vm(4, 512, 1024),
            vm(256, 1024, dtype=F32),
            vm(512, 256, dtype=F32),
            vm(512, 256, dtype=F32),
            vm(4, 4, 4, 32, 256),
            vm(4, 4, 4, 32, 256),
            vm(2, 4, 2, 32, 256),
            vm(2, 4, 4, 32, 256),
            vm(2, 2, 2, 32, 256),
            vm(2, 4, 2, 32, 256),
            vm(2, 4, 4, 32, 256),
            vm(2, 2, 2, 32, 256),
            vm(2, 4, 32, 256),
            vm(2, 4, 32, 256),
            vm(2, 4, 32, 256),
            vm(2, 4, 32, 256),
            vm(2, 4, 32, 256),
            vm(2, 4, 32, 256),
            pltpu.SemaphoreType.DMA((4,)),
            pltpu.SemaphoreType.DMA((SENDS,)),
            pltpu.SemaphoreType.DMA((COPIES,)),
        ],
        compiler_params=pltpu.CompilerParams(
            collective_id=0, has_side_effects=True, vmem_limit_bytes=66600000
        ),
    )(doc_lengths, fold_order, queries, keys, values, d_out)
    return pl.pallas_call(
        leave,
        out_shape=tuple(jax.ShapeDtypeStruct(g.shape, g.dtype) for g in grads),
        in_specs=[vmem] * 3,
        out_specs=(hbm,) * 3,
        scratch_shapes=[pltpu.SemaphoreType.DMA((3,))],
        compiler_params=pltpu.CompilerParams(vmem_limit_bytes=1024 * 1024),
    )(*grads)


def solution(mesh):
    in_specs = (
        P("head", "seq", None),
        P(None, "seq", None),
        P(None, "seq", None),
        P("head", "seq", None),
        P(),
        P(),
    )
    out_specs = (
        P("head", "seq", None),
        P(None, ("seq", "head"), None),
        P(None, ("seq", "head"), None),
    )
    return jax.shard_map(
        per_device, mesh=mesh, in_specs=in_specs, out_specs=out_specs, check_vma=False
    )
```

```python
import jax
import jax.numpy as jnp
from jax import lax
from jax.experimental import pallas as pl
from jax.experimental.pallas import tpu as pltpu
from jax.sharding import PartitionSpec as P

MESH = pl.DeviceIdType.MESH
LOG2E = 1.4426950408889634
MASKED = -1e30
BLOCK = 256
F32 = jnp.float32
BF16 = jnp.bfloat16
ROW_HEADS = 8
COPIES = 63
SENDS = 32


def nt(a, b):
    return lax.dot_general(a, b, (((1,), (1,)), ((), ())), preferred_element_type=F32)


def nn(a, b):
    return lax.dot_general(a, b, (((1,), (0,)), ((), ())), preferred_element_type=F32)


def tn(a, b):
    return lax.dot_general(a, b, (((0,), (0,)), ((), ())), preferred_element_type=F32)


def kernel(
    lengths, fold, q_hbm, k_hbm, v_hbm, do_hbm,
    dq_out, dk_out, dv_out,
    qv, dov, qs, qst, dot_, kv, sc, dp, stat, stat2, dsb, dqt, dqs, dqr,
    ak, av, rk, fk, dk2, rv, fv, dv2, zv, fev, yk, fgk, xs, rx,
    local_sem, send_sem, recv_sem,
):
    s = lax.axis_index("seq")
    h = lax.axis_index("head")
    y, c = lax.div(s, 2), lax.rem(s, 2)
    x, z = lax.div(h, 4), lax.rem(h, 4)
    row = lax.div(h, ROW_HEADS)

    def around(v, k):
        return lax.rem(v + (k % 4), 4)

    partner = {"seq": 2 * y + (1 - c), "head": h}
    yp = {"seq": 2 * around(y, 1) + c, "head": h}
    ym = {"seq": 2 * around(y, -1) + c, "head": h}
    yf = {"seq": 2 * around(y, 2) + c, "head": h}
    zp = {"seq": s, "head": 4 * x + around(z, 1)}
    zm = {"seq": s, "head": 4 * x + around(z, -1)}
    diag = {
        (i, j): {"seq": 2 * around(y, i) + c, "head": 4 * x + around(z, j)} for i in (-1, 1) for j in (-1, 1)
    }
    xo = [{"seq": s, "head": 4 * around(x, k) + z} for k in (1, 2, 3)]

    mine = pl.ds(pl.multiple_of(512 * c, 512), 512)
    theirs = pl.ds(pl.multiple_of(512 * (1 - c), 512), 512)

    loads = [
        pltpu.make_async_copy(v_hbm.at[row], kv.at[y, 1], local_sem.at[0]),
        pltpu.make_async_copy(k_hbm.at[row], kv.at[y, 0], local_sem.at[1]),
        pltpu.make_async_copy(q_hbm.at[0], qv.at[mine], local_sem.at[2]),
        pltpu.make_async_copy(do_hbm.at[0], dov.at[mine], local_sem.at[3]),
    ]
    for cp in loads:
        cp.start()

    barrier = pltpu.get_barrier_semaphore()
    peers = [partner, yp, ym, yf, zp, zm] + list(diag.values()) + xo
    for peer in peers:
        pl.semaphore_signal(barrier, inc=1, device_id=peer, device_id_type=MESH)
    pl.semaphore_wait(barrier, len(peers))

    started = []

    used = [0]

    def take():
        used[0] += 1
        return used[0] - 1

    def remote(src, dst, device, i, r):
        return pltpu.make_async_remote_copy(
            src_ref=src, dst_ref=dst, send_sem=send_sem.at[i], recv_sem=recv_sem.at[r],
            device_id=device, device_id_type=MESH,
        )

    def send(src, dst, device, group=None):
        i = len(started)
        if i >= SENDS:
            started[i - SENDS].wait_send()
        cp = remote(src, dst, device, i % SENDS, take() if group is None else group)
        cp.start()
        started.append(cp)
        return cp

    def wait_group(whole, group):
        remote(whole, whole, partner, 0, group).wait_recv()

    def same(ref, device):
        return send(ref, ref, device)

    def chip(k):
        return around(y, k)

    zq = 128 * z

    def vquarter(yi, zi, lo, n):
        return kv.at[yi, 1, pl.ds(pl.multiple_of(128 * zi + lo, 64), n)]

    low, high = pl.ds(0, 128), pl.ds(128, 128)
    xb = lax.rem(x, 2)
    xpair = {"seq": s, "head": 4 * (x + 1 - 2 * xb) + z}

    def khalf(yi, lo, n):
        return kv.at[yi, 0, pl.ds(pl.multiple_of(256 + 128 * xb + lo, 64), n)]

    loads[0].wait()
    v_p = same(vquarter(y, z, 0, 128), yp)
    v_m = same(vquarter(y, z, 0, 128), ym)
    v_f = same(vquarter(y, z, 0, 128), yf)
    loads[2].wait()
    q_pair = same(qv.at[mine], partner)
    loads[3].wait()
    do_pair = same(dov.at[mine], partner)

    lane = lax.broadcasted_iota(jnp.int32, (1, 1024), 1)
    pos = lane + fold[4 * y] * BLOCK
    for b in (1, 2, 3):
        pos = jnp.where(lane < BLOCK * b, pos, lane + (fold[4 * y + b] - b) * BLOCK)
    first = jnp.zeros((1, 1024), jnp.int32)
    at = jnp.int32(0)
    for d in range(8):
        first = jnp.where(pos >= at, at, first)
        at = at + lengths[row, d]
    rows = lax.broadcasted_iota(jnp.int32, (BLOCK, 1024), 0)
    stat[0:1, :] = jnp.full((1, 1024), MASKED, F32)
    stat[1:3, :] = jnp.zeros((2, 1024), F32)
    stat[3:4, :] = jnp.full((1, 1024), MASKED, F32)
    stat[4:8, :] = jnp.zeros((4, 1024), F32)
    q_pair.wait_recv()
    qs[...] = (qv[...].astype(F32) * 0.0625).astype(BF16)
    qst[...] = jnp.transpose(qs[...])
    do_pair.wait_recv()
    dot_[...] = jnp.transpose(dov[...])

    offsets = (2, 1, -1, 0)

    parts = [pl.ds(half * BLOCK, BLOCK) for half in (0, 1)]

    def scores(j, half, off=0, n=BLOCK):
        yi = chip(offsets[j])
        part = pl.ds(pl.multiple_of(half * BLOCK + off, 128), n)
        base = fold[4 * yi + 2 * c + half] * BLOCK + off
        raw = nn(kv[yi, 0, part, :], qst[...])
        ok = (rows[:n] >= first - base) & (rows[:n] <= pos - base)
        s2 = jnp.where(ok, raw * LOG2E, MASKED)
        sc[j, part, :] = s2
        stat[0:1, :] = jnp.maximum(stat[0:1, :], jnp.max(s2, axis=0, keepdims=True))

    def probs(j):
        yi = chip(offsets[j])
        m = stat[0:1, :]
        alpha = jnp.exp2(stat[3:4, :] - m)
        total = stat[1:2, :] * alpha
        dot = stat[2:3, :] * alpha
        for part in parts:
            gp = nn(kv[yi, 1, part, :], dot_[...])
            dp[j, part, :] = gp
            e = jnp.exp2(sc[j, part, :] - m)
            total = total + jnp.sum(e, axis=0, keepdims=True)
            dot = dot + jnp.sum(e * gp, axis=0, keepdims=True)
        stat[1:2, :] = total
        stat[2:3, :] = dot
        stat[3:4, :] = m

    shares, relays = {}, {}

    def share(k):
        shares[k] = (
            same(vquarter(chip(k), z, 0, 128), zp),
            same(vquarter(chip(k), z, 0, 128), zm),
        )

    def relay(k):
        shares[k][0].wait_recv()
        a = same(vquarter(chip(k), around(z, -1), 0, 64), zp)
        shares[k][1].wait_recv()
        relays[k] = a, same(vquarter(chip(k), around(z, 1), 64, 64), zm)

    loads[1].wait()
    kx_p = same(khalf(y, 0, 128), yp)
    kx_m = same(khalf(y, 0, 128), ym)
    ka_p = same(kv.at[y, 0, low], yp)
    kb_m = same(kv.at[y, 0, high], ym)
    scores(3, 0)
    scores(3, 1)
    v_p.wait_recv()
    share(-1)
    v_m.wait_recv()
    share(1)
    kb_p = same(kv.at[y, 0, high], yp)
    ka_m = same(kv.at[y, 0, low], ym)
    v_f.wait_recv()
    share(2)
    probs(3)
    cross = {}
    kx_p.wait_recv()
    x2a = same(khalf(chip(-1), 0, 64), yp)
    cross[-1] = same(khalf(chip(-1), 0, 128), xpair)
    kx_m.wait_recv()
    x2b = same(khalf(chip(1), 64, 64), ym)
    cross[1] = same(khalf(chip(1), 0, 128), xpair)
    scores(2, 1, 128 * xb, 128)
    scores(1, 1, 128 * xb, 128)
    ka_p.wait_recv()
    k2a = same(kv.at[chip(-1), 0, low], yp)
    kb_m.wait_recv()
    k2b = same(kv.at[chip(1), 0, high], ym)
    scores(2, 0, 0, 128)
    relay(-1)
    scores(1, 0, 128, 128)
    relay(1)
    kb_p.wait_recv()
    scores(2, 0, 128, 128)
    x2a.wait_recv()
    x2b.wait_recv()
    cross[2] = same(khalf(chip(2), 0, 128), xpair)
    relay(2)
    ka_m.wait_recv()
    scores(1, 0, 0, 128)
    cross[-1].wait_recv()
    scores(2, 1, 128 * (1 - xb), 128)
    cross[1].wait_recv()
    scores(1, 1, 128 * (1 - xb), 128)
    k2a.wait_recv()
    k2b.wait_recv()
    scores(0, 0)
    for r in relays[-1]:
        r.wait_recv()
    probs(2)
    for r in relays[1]:
        r.wait_recv()
    probs(1)
    cross[2].wait_recv()
    scores(0, 1)
    for r in relays[2]:
        r.wait_recv()
    probs(0)

    stat_pair = send(stat, stat2, partner)
    stat_pair.wait_recv()
    top = jnp.maximum(stat[0:1, :], stat2[0:1, :])
    w1 = jnp.exp2(stat[0:1, :] - top)
    w2 = jnp.exp2(stat2[0:1, :] - top)
    total = stat[1:2, :] * w1 + stat2[1:2, :] * w2
    lse = top + jnp.log2(total)
    gdot = (stat[2:3, :] * w1 + stat2[2:3, :] * w2) / total

    def backward(j):
        out = []
        for half in (0, 1):
            part = pl.ds(half * BLOCK, BLOCK)
            p = jnp.exp2(sc[j, part, :] - lse)
            ds = (p * (dp[j, part, :] - gdot)).astype(BF16)
            dsb[j, part, :] = ds
            out.append((nn(ds, qs[...]), nn(p.astype(BF16), dov[...])))
        return out

    def queries():
        acc = tn(kv[chip(offsets[0]), 0], dsb[0])
        for j in (1, 2, 3):
            acc = acc + tn(kv[chip(offsets[j]), 0], dsb[j])
        return acc

    def up(v):
        return v.astype(F32)

    pieces = [(xp, zi) for xp in range(4) for zi in range(4)]
    place = [lax.rem(zi - z + 5, 4) for zi in range(4)]
    lo, hi = pl.ds(0, 2), pl.ds(2, 2)
    near, far = pl.ds(0, 3), 3
    kc, vc = {}, {}
    vgroup = [take() for _ in range(4)]
    kgroup = take()

    def values_second(j):
        vc[j, 1].wait_recv()
        av[j, 2, 0:2] = (up(av[j, 2, 0:2]) + up(rv[0, j])).astype(BF16)
        if j == 0:
            vc[j, 4] = send(av.at[j, 2, lo], dv2.at[0, 0], diag[1, 1], vgroup[0])
        else:
            vc[j, 4] = send(av.at[j, 2, lo], fv.at[0, j, lo], zp, vgroup[j])
        vc[j, 2].wait_recv()
        av[j, 0, 2:4] = (up(av[j, 0, 2:4]) + up(rv[1, j])).astype(BF16)
        if j == 0:
            vc[j, 6] = send(av.at[j, 0, hi], dv2.at[1, 0], diag[-1, -1], vgroup[0])
        else:
            vc[j, 6] = send(av.at[j, 0, hi], fv.at[1, j, hi], zm, vgroup[j])

    def values_early():
        vc[0, 5].wait_recv()
        av[0, 1, 0:2] = (up(av[0, 1, 0:2]) + up(fv[1, 0, 0:2])).astype(BF16)
        vc[0, 7] = send(av.at[0, 1, lo], dv2.at[0, 1], yp, vgroup[0])
        vc[0, 3].wait_recv()
        av[0, 1, 2:4] = (up(av[0, 1, 2:4]) + up(fv[0, 0, 2:4])).astype(BF16)
        vc[0, 8] = send(av.at[0, 1, hi], dv2.at[1, 1], ym, vgroup[0])

    def keys_early():
        kc[5].wait_recv()
        ak[3, 3, 0:2] = (up(ak[3, 3, 0:2]) + up(fk[1, 3, 0:2])).astype(BF16)
        kc[17] = send(ak.at[3, far, lo], dk2.at[0, 1], zp, kgroup)
        kc[3].wait_recv()
        ak[3, 3, 2:4] = (up(ak[3, 3, 2:4]) + up(fk[0, 3, 2:4])).astype(BF16)
        kc[18] = send(ak.at[3, far, hi], dk2.at[1, 1], zm, kgroup)

    def block(j):
        for half, (gk_, gv) in enumerate(backward(j)):
            gk_, gv = gk_.astype(BF16), gv.astype(BF16)
            for xp, zi in pieces:
                r0 = (4 * xp + zi) * 32 - half * BLOCK
                if 0 <= r0 < BLOCK:
                    ak[j, place[zi], xp] = gk_[r0 : r0 + 32, :]
                    av[j, place[zi], xp] = gv[r0 : r0 + 32, :]
        for half in (0, 1):
            at_ = (lo, hi)[half]
            to = (zp, zm)[half]
            vc[j, 1 + half] = send(av.at[j, far, at_], rv.at[half, j], to)
            if j == 0:
                kc[1 + half] = send(ak.at[0, pl.ds(0, 4), at_], rk.at[half], (yp, ym)[half])
            if j == 1 and half == 1:
                kc[3] = send(ak.at[1, pl.ds(0, 4), hi], fk.at[0, pl.ds(0, 4), hi], yp)
            if j == 2 and half == 0:
                kc[5] = send(ak.at[2, pl.ds(0, 4), lo], fk.at[1, pl.ds(0, 4), lo], ym)
            if half == 0:
                vc[j, 5] = send(av.at[j, 0, lo], fv.at[1, j, lo], zm, vgroup[j] if j else None)
            else:
                vc[j, 3] = send(av.at[j, 2, hi], fv.at[0, j, hi], zp, vgroup[j] if j else None)

    block(0)
    block(1)
    block(2)
    block(3)
    values_second(0)
    kc[1].wait_recv()
    ak[1, :, 0:2] = (up(ak[1, :, 0:2]) + up(rk[0])).astype(BF16)
    kc[14] = send(ak.at[1, far, lo], dk2.at[0, 0], diag[1, 1], kgroup)
    kc[4] = send(ak.at[1, near, lo], fk.at[0, pl.ds(0, 3), lo], yp)
    kc[2].wait_recv()
    ak[2, :, 2:4] = (up(ak[2, :, 2:4]) + up(rk[1])).astype(BF16)
    kc[16] = send(ak.at[2, far, hi], dk2.at[1, 0], diag[-1, -1], kgroup)
    kc[6] = send(ak.at[2, near, hi], fk.at[1, pl.ds(0, 3), hi], ym)
    values_second(1)
    values_early()
    values_second(2)
    values_second(3)

    keys_early()
    dqt[...] = queries()
    dqs[...] = jnp.transpose(dqt[:, theirs])
    dq_pair = send(dqs, dqr, partner)

    def values_along_z(j):
        wait_group(fv.at[pl.ds(0, 2), j], vgroup[j])
        return up(av[j, 1]) + up(fv[0, j]) + up(fv[1, j])

    wait_group(dv2, vgroup[0])
    ec = {}
    w = values_along_z(1)
    zv[0, 0:2] = (w[0:2] + up(dv2[0, 0]) + up(dv2[0, 1])).astype(BF16)
    zv[0, 2:4] = w[2:4].astype(BF16)
    ec[0] = send(zv.at[0], fev.at[0], yp)
    w = values_along_z(2)
    zv[1, 0:2] = w[0:2].astype(BF16)
    zv[1, 2:4] = (w[2:4] + up(dv2[1, 0]) + up(dv2[1, 1])).astype(BF16)
    ec[1] = send(zv.at[1], fev.at[1], ym)

    for i in (4, 6):
        kc[i].wait_recv()

    def keys_along_y(q):
        return up(ak[3, q]) + up(fk[0, q]) + up(fk[1, q])

    wait_group(dk2, kgroup)
    gc = {}
    w = keys_along_y(2)
    yk[0, 0:2] = (w[0:2] + up(dk2[0, 0]) + up(dk2[0, 1])).astype(BF16)
    yk[0, 2:4] = w[2:4].astype(BF16)
    gc[0] = send(yk.at[0], fgk.at[0], zp)
    w = keys_along_y(0)
    yk[1, 0:2] = w[0:2].astype(BF16)
    yk[1, 2:4] = (w[2:4] + up(dk2[1, 0]) + up(dk2[1, 1])).astype(BF16)
    gc[1] = send(yk.at[1], fgk.at[1], zm)

    w = values_along_z(3)
    for cp in ec.values():
        cp.wait_recv()
    xs[1] = (w + up(fev[0]) + up(fev[1])).astype(BF16)
    xc = []
    for k in (2, 1, 3):
        xc.append(send(xs.at[1, around(x, k)], rx.at[1, x], xo[k - 1]))
    dq_pair.wait_recv()
    dq_out[0] = ((jnp.transpose(dqt[:, mine]) + dqr[...]) * 0.0625).astype(BF16)
    for cp in gc.values():
        cp.wait_recv()
    xs[0] = (keys_along_y(1) + up(fgk[0]) + up(fgk[1])).astype(BF16)
    for k in (2, 1, 3):
        xc.append(send(xs.at[0, around(x, k)], rx.at[0, x], xo[k - 1]))
    rx[0, x] = xs[0, x]
    rx[1, x] = xs[1, x]
    for cp in xc:
        cp.wait_recv()
    for r in (0, 1):
        dk_out[r] = up(rx[0, 2 * r]) + up(rx[0, 2 * r + 1])
        dv_out[r] = up(rx[1, 2 * r]) + up(rx[1, 2 * r + 1])
    for cp in started[-SENDS:]:
        cp.wait_send()
    assert used[0] == COPIES, used[0]


def leave(a, b, c, a_out, b_out, c_out, sem):
    moves = [pltpu.make_async_copy(src, dst, sem.at[i]) for i, (src, dst) in enumerate(((a, a_out), (b, b_out), (c, c_out)))]
    for cp in moves:
        cp.start()
    for cp in moves:
        cp.wait()


def per_device(queries, keys, values, d_out, doc_lengths, fold_order):
    hbm = pl.BlockSpec(memory_space=pl.ANY)
    vmem = pl.BlockSpec(memory_space=pltpu.VMEM)
    smem = pl.BlockSpec(memory_space=pltpu.SMEM)

    def vm(*shape, dtype=BF16):
        return pltpu.VMEM(shape, dtype)

    grads = pl.pallas_call(
        kernel,
        out_shape=(
            pltpu.VMEM((1, 512, 256), BF16),
            pltpu.VMEM((2, 32, 256), F32),
            pltpu.VMEM((2, 32, 256), F32),
        ),
        in_specs=[smem, smem, hbm, hbm, hbm, hbm],
        out_specs=(vmem, vmem, vmem),
        scratch_shapes=[
            vm(1024, 256),
            vm(1024, 256),
            vm(1024, 256),
            vm(256, 1024),
            vm(256, 1024),
            vm(4, 2, 512, 256),
            vm(4, 512, 1024, dtype=F32),
            vm(4, 512, 1024, dtype=F32),
            vm(8, 1024, dtype=F32),
            vm(8, 1024, dtype=F32),
            vm(4, 512, 1024),
            vm(256, 1024, dtype=F32),
            vm(512, 256, dtype=F32),
            vm(512, 256, dtype=F32),
            vm(4, 4, 4, 32, 256),
            vm(4, 4, 4, 32, 256),
            vm(2, 4, 2, 32, 256),
            vm(2, 4, 4, 32, 256),
            vm(2, 2, 2, 32, 256),
            vm(2, 4, 2, 32, 256),
            vm(2, 4, 4, 32, 256),
            vm(2, 2, 2, 32, 256),
            vm(2, 4, 32, 256),
            vm(2, 4, 32, 256),
            vm(2, 4, 32, 256),
            vm(2, 4, 32, 256),
            vm(2, 4, 32, 256),
            vm(2, 4, 32, 256),
            pltpu.SemaphoreType.DMA((4,)),
            pltpu.SemaphoreType.DMA((SENDS,)),
            pltpu.SemaphoreType.DMA((COPIES,)),
        ],
        compiler_params=pltpu.CompilerParams(
            collective_id=0, has_side_effects=True, vmem_limit_bytes=66600000
        ),
    )(doc_lengths, fold_order, queries, keys, values, d_out)
    return pl.pallas_call(
        leave,
        out_shape=tuple(jax.ShapeDtypeStruct(g.shape, g.dtype) for g in grads),
        in_specs=[vmem] * 3,
        out_specs=(hbm,) * 3,
        scratch_shapes=[pltpu.SemaphoreType.DMA((3,))],
        compiler_params=pltpu.CompilerParams(vmem_limit_bytes=1024 * 1024),
    )(*grads)


def solution(mesh):
    in_specs = (
        P("head", "seq", None),
        P(None, "seq", None),
        P(None, "seq", None),
        P("head", "seq", None),
        P(),
        P(),
    )
    out_specs = (
        P("head", "seq", None),
        P(None, ("seq", "head"), None),
        P(None, ("seq", "head"), None),
    )
    return jax.shard_map(
        per_device, mesh=mesh, in_specs=in_specs, out_specs=out_specs, check_vma=False
    )
```

```python
import jax
import jax.numpy as jnp
from jax import lax
from jax.experimental import pallas as pl
from jax.experimental.pallas import tpu as pltpu
from jax.sharding import PartitionSpec as P

MESH = pl.DeviceIdType.MESH
LOG2E = 1.4426950408889634
MASKED = -1e30
BLOCK = 256
F32 = jnp.float32
BF16 = jnp.bfloat16
ROW_HEADS = 8
COPIES = 78
SENDS = 40


def nt(a, b):
    return lax.dot_general(a, b, (((1,), (1,)), ((), ())), preferred_element_type=F32)


def nn(a, b):
    return lax.dot_general(a, b, (((1,), (0,)), ((), ())), preferred_element_type=F32)


def tn(a, b):
    return lax.dot_general(a, b, (((0,), (0,)), ((), ())), preferred_element_type=F32)


def kernel(
    lengths, fold, q_hbm, k_hbm, v_hbm, do_hbm,
    dq_out, dk_out, dv_out,
    qv, dov, qs, qst, dot_, kv, sc, dp, stat, stat2, dsb, dqt, dqs, dqr,
    ak, av, rk, fk, dk2, rv, fv, dv2, zv, fev, yk, fgk, xs, rx,
    local_sem, send_sem, recv_sem,
):
    s = lax.axis_index("seq")
    h = lax.axis_index("head")
    y, c = lax.div(s, 2), lax.rem(s, 2)
    x, z = lax.div(h, 4), lax.rem(h, 4)
    row = lax.div(h, ROW_HEADS)

    def around(v, k):
        return lax.rem(v + (k % 4), 4)

    partner = {"seq": 2 * y + (1 - c), "head": h}
    yp = {"seq": 2 * around(y, 1) + c, "head": h}
    ym = {"seq": 2 * around(y, -1) + c, "head": h}
    yf = {"seq": 2 * around(y, 2) + c, "head": h}
    zp = {"seq": s, "head": 4 * x + around(z, 1)}
    zm = {"seq": s, "head": 4 * x + around(z, -1)}
    diag = {
        (i, j): {"seq": 2 * around(y, i) + c, "head": 4 * x + around(z, j)} for i in (-1, 1) for j in (-1, 1)
    }
    xo = [{"seq": s, "head": 4 * around(x, k) + z} for k in (1, 2, 3)]

    mine = pl.ds(pl.multiple_of(512 * c, 512), 512)
    theirs = pl.ds(pl.multiple_of(512 * (1 - c), 512), 512)

    loads = [
        pltpu.make_async_copy(v_hbm.at[row], kv.at[y, 1], local_sem.at[0]),
        pltpu.make_async_copy(k_hbm.at[row], kv.at[y, 0], local_sem.at[1]),
        pltpu.make_async_copy(q_hbm.at[0], qv.at[mine], local_sem.at[2]),
        pltpu.make_async_copy(do_hbm.at[0], dov.at[mine], local_sem.at[3]),
    ]
    for cp in loads:
        cp.start()

    barrier = pltpu.get_barrier_semaphore()
    peers = [partner, yp, ym, yf, zp, zm] + list(diag.values()) + xo
    for peer in peers:
        pl.semaphore_signal(barrier, inc=1, device_id=peer, device_id_type=MESH)
    pl.semaphore_wait(barrier, len(peers))

    started = []

    def send(src, dst, device):
        i = len(started)
        if i >= SENDS:
            started[i - SENDS].wait_send()
        cp = pltpu.make_async_remote_copy(
            src_ref=src, dst_ref=dst, send_sem=send_sem.at[i % SENDS], recv_sem=recv_sem.at[i],
            device_id=device, device_id_type=MESH,
        )
        cp.start()
        started.append(cp)
        return cp

    def same(ref, device):
        return send(ref, ref, device)

    def chip(k):
        return around(y, k)

    zq = 128 * z

    def vquarter(yi, zi, lo, n):
        return kv.at[yi, 1, pl.ds(pl.multiple_of(128 * zi + lo, 64), n)]

    low, high = pl.ds(0, 128), pl.ds(128, 128)
    xb = lax.rem(x, 2)
    xpair = {"seq": s, "head": 4 * (x + 1 - 2 * xb) + z}

    def khalf(yi, lo, n):
        return kv.at[yi, 0, pl.ds(pl.multiple_of(256 + 128 * xb + lo, 64), n)]

    loads[0].wait()
    v_p = same(vquarter(y, z, 0, 128), yp)
    v_m = same(vquarter(y, z, 0, 128), ym)
    v_f = same(vquarter(y, z, 0, 128), yf)
    loads[2].wait()
    q_pair = same(qv.at[mine], partner)
    loads[3].wait()
    do_pair = same(dov.at[mine], partner)

    lane = lax.broadcasted_iota(jnp.int32, (1, 1024), 1)
    pos = lane + fold[4 * y] * BLOCK
    for b in (1, 2, 3):
        pos = jnp.where(lane < BLOCK * b, pos, lane + (fold[4 * y + b] - b) * BLOCK)
    first = jnp.zeros((1, 1024), jnp.int32)
    at = jnp.int32(0)
    for d in range(8):
        first = jnp.where(pos >= at, at, first)
        at = at + lengths[row, d]
    rows = lax.broadcasted_iota(jnp.int32, (BLOCK, 1024), 0)
    stat[0:1, :] = jnp.full((1, 1024), MASKED, F32)
    stat[1:3, :] = jnp.zeros((2, 1024), F32)
    stat[3:4, :] = jnp.full((1, 1024), MASKED, F32)
    stat[4:8, :] = jnp.zeros((4, 1024), F32)
    q_pair.wait_recv()
    qs[...] = (qv[...].astype(F32) * 0.0625).astype(BF16)
    qst[...] = jnp.transpose(qs[...])
    do_pair.wait_recv()
    dot_[...] = jnp.transpose(dov[...])

    offsets = (2, 1, -1, 0)

    parts = [pl.ds(half * BLOCK, BLOCK) for half in (0, 1)]

    def scores(j, half, off=0, n=BLOCK):
        yi = chip(offsets[j])
        part = pl.ds(pl.multiple_of(half * BLOCK + off, 128), n)
        base = fold[4 * yi + 2 * c + half] * BLOCK + off
        raw = nn(kv[yi, 0, part, :], qst[...])
        ok = (rows[:n] >= first - base) & (rows[:n] <= pos - base)
        s2 = jnp.where(ok, raw * LOG2E, MASKED)
        sc[j, part, :] = s2
        stat[0:1, :] = jnp.maximum(stat[0:1, :], jnp.max(s2, axis=0, keepdims=True))

    def probs(j):
        yi = chip(offsets[j])
        m = stat[0:1, :]
        alpha = jnp.exp2(stat[3:4, :] - m)
        total = stat[1:2, :] * alpha
        dot = stat[2:3, :] * alpha
        dp[j] = nn(kv[yi, 1], dot_[...])
        for part in parts:
            gp = dp[j, part, :]
            e = jnp.exp2(sc[j, part, :] - m)
            total = total + jnp.sum(e, axis=0, keepdims=True)
            dot = dot + jnp.sum(e * gp, axis=0, keepdims=True)
        stat[1:2, :] = total
        stat[2:3, :] = dot
        stat[3:4, :] = m

    shares, relays = {}, {}

    def share(k):
        shares[k] = (
            same(vquarter(chip(k), z, 0, 128), zp),
            same(vquarter(chip(k), z, 0, 128), zm),
        )

    def relay(k):
        shares[k][0].wait_recv()
        a = same(vquarter(chip(k), around(z, -1), 0, 64), zp)
        shares[k][1].wait_recv()
        relays[k] = a, same(vquarter(chip(k), around(z, 1), 64, 64), zm)

    loads[1].wait()
    kx_p = same(khalf(y, 0, 128), yp)
    kx_m = same(khalf(y, 0, 128), ym)
    ka_p = same(kv.at[y, 0, low], yp)
    kb_m = same(kv.at[y, 0, high], ym)
    scores(3, 0)
    scores(3, 1)
    v_p.wait_recv()
    share(-1)
    v_m.wait_recv()
    share(1)
    kb_p = same(kv.at[y, 0, high], yp)
    ka_m = same(kv.at[y, 0, low], ym)
    v_f.wait_recv()
    share(2)
    probs(3)
    cross = {}
    kx_p.wait_recv()
    x2a = same(khalf(chip(-1), 0, 64), yp)
    cross[-1] = same(khalf(chip(-1), 0, 128), xpair)
    kx_m.wait_recv()
    x2b = same(khalf(chip(1), 64, 64), ym)
    cross[1] = same(khalf(chip(1), 0, 128), xpair)
    scores(2, 1, 128 * xb, 128)
    scores(1, 1, 128 * xb, 128)
    ka_p.wait_recv()
    k2a = same(kv.at[chip(-1), 0, low], yp)
    kb_m.wait_recv()
    k2b = same(kv.at[chip(1), 0, high], ym)
    scores(2, 0, 0, 128)
    relay(-1)
    scores(1, 0, 128, 128)
    relay(1)
    kb_p.wait_recv()
    scores(2, 0, 128, 128)
    x2a.wait_recv()
    x2b.wait_recv()
    cross[2] = same(khalf(chip(2), 0, 128), xpair)
    relay(2)
    ka_m.wait_recv()
    scores(1, 0, 0, 128)
    cross[-1].wait_recv()
    scores(2, 1, 128 * (1 - xb), 128)
    cross[1].wait_recv()
    scores(1, 1, 128 * (1 - xb), 128)
    k2a.wait_recv()
    k2b.wait_recv()
    scores(0, 0)
    for r in relays[-1]:
        r.wait_recv()
    probs(2)
    for r in relays[1]:
        r.wait_recv()
    probs(1)
    cross[2].wait_recv()
    scores(0, 1)
    for r in relays[2]:
        r.wait_recv()
    probs(0)

    stat_pair = send(stat, stat2, partner)
    stat_pair.wait_recv()
    top = jnp.maximum(stat[0:1, :], stat2[0:1, :])
    w1 = jnp.exp2(stat[0:1, :] - top)
    w2 = jnp.exp2(stat2[0:1, :] - top)
    total = stat[1:2, :] * w1 + stat2[1:2, :] * w2
    lse = top + jnp.log2(total)
    gdot = (stat[2:3, :] * w1 + stat2[2:3, :] * w2) / total

    def backward(j):
        p = jnp.exp2(sc[j] - lse)
        ds = (p * (dp[j] - gdot)).astype(BF16)
        dsb[j] = ds
        return nn(ds, qs[...]), nn(p.astype(BF16), dov[...])

    def queries():
        acc = tn(kv[chip(offsets[0]), 0], dsb[0])
        for j in (1, 2, 3):
            acc = acc + tn(kv[chip(offsets[j]), 0], dsb[j])
        return acc

    def up(v):
        return v.astype(F32)

    pieces = [(xp, zi) for xp in range(4) for zi in range(4)]
    place = [lax.rem(zi - z + 5, 4) for zi in range(4)]
    lo, hi = pl.ds(0, 2), pl.ds(2, 2)
    near, far = pl.ds(0, 3), 3
    kc, vc = {}, {}

    def values_second(j):
        vc[j, 1].wait_recv()
        av[j, 2, 0:2] = (up(av[j, 2, 0:2]) + up(rv[0, j])).astype(BF16)
        if j == 0:
            vc[j, 4] = send(av.at[j, 2, lo], dv2.at[0, 0], diag[1, 1])
        else:
            vc[j, 4] = send(av.at[j, 2, lo], fv.at[0, j, lo], zp)
        vc[j, 2].wait_recv()
        av[j, 0, 2:4] = (up(av[j, 0, 2:4]) + up(rv[1, j])).astype(BF16)
        if j == 0:
            vc[j, 6] = send(av.at[j, 0, hi], dv2.at[1, 0], diag[-1, -1])
        else:
            vc[j, 6] = send(av.at[j, 0, hi], fv.at[1, j, hi], zm)

    def values_early():
        vc[0, 5].wait_recv()
        av[0, 1, 0:2] = (up(av[0, 1, 0:2]) + up(fv[1, 0, 0:2])).astype(BF16)
        vc[0, 7] = send(av.at[0, 1, lo], dv2.at[0, 1], yp)
        vc[0, 3].wait_recv()
        av[0, 1, 2:4] = (up(av[0, 1, 2:4]) + up(fv[0, 0, 2:4])).astype(BF16)
        vc[0, 8] = send(av.at[0, 1, hi], dv2.at[1, 1], ym)

    def keys_early():
        kc[5].wait_recv()
        ak[3, 3, 0:2] = (up(ak[3, 3, 0:2]) + up(fk[1, 3, 0:2])).astype(BF16)
        kc[17] = send(ak.at[3, far, lo], dk2.at[0, 1], zp)
        kc[3].wait_recv()
        ak[3, 3, 2:4] = (up(ak[3, 3, 2:4]) + up(fk[0, 3, 2:4])).astype(BF16)
        kc[18] = send(ak.at[3, far, hi], dk2.at[1, 1], zm)

    def block(j):
        gk_, gv = backward(j)
        gk_, gv = gk_.astype(BF16), gv.astype(BF16)
        for xp, zi in pieces:
            r0 = (4 * xp + zi) * 32
            ak[j, place[zi], xp] = gk_[r0 : r0 + 32, :]
            av[j, place[zi], xp] = gv[r0 : r0 + 32, :]
        for half in (0, 1):
            at_ = (lo, hi)[half]
            to = (zp, zm)[half]
            vc[j, 1 + half] = send(av.at[j, far, at_], rv.at[half, j], to)
            if j == 0:
                kc[1 + half] = send(ak.at[0, pl.ds(0, 4), at_], rk.at[half], (yp, ym)[half])
            if j == 1 and half == 1:
                kc[3] = send(ak.at[1, pl.ds(0, 4), hi], fk.at[0, pl.ds(0, 4), hi], yp)
            if j == 2 and half == 0:
                kc[5] = send(ak.at[2, pl.ds(0, 4), lo], fk.at[1, pl.ds(0, 4), lo], ym)
            if half == 0:
                vc[j, 5] = send(av.at[j, 0, lo], fv.at[1, j, lo], zm)
            else:
                vc[j, 3] = send(av.at[j, 2, hi], fv.at[0, j, hi], zp)

    block(0)
    block(1)
    block(2)
    block(3)
    values_second(0)
    kc[1].wait_recv()
    ak[1, :, 0:2] = (up(ak[1, :, 0:2]) + up(rk[0])).astype(BF16)
    kc[14] = send(ak.at[1, far, lo], dk2.at[0, 0], diag[1, 1])
    kc[4] = send(ak.at[1, near, lo], fk.at[0, pl.ds(0, 3), lo], yp)
    kc[2].wait_recv()
    ak[2, :, 2:4] = (up(ak[2, :, 2:4]) + up(rk[1])).astype(BF16)
    kc[16] = send(ak.at[2, far, hi], dk2.at[1, 0], diag[-1, -1])
    kc[6] = send(ak.at[2, near, hi], fk.at[1, pl.ds(0, 3), hi], ym)
    values_second(1)
    values_early()
    values_second(2)
    values_second(3)

    keys_early()
    dqt[...] = queries()
    dqs[...] = jnp.transpose(dqt[:, theirs])
    dq_pair = send(dqs, dqr, partner)

    def values_along_z(j):
        for i in (3, 4, 5, 6):
            vc[j, i].wait_recv()
        return up(av[j, 1]) + up(fv[0, j]) + up(fv[1, j])

    for i in (4, 6, 7, 8):
        vc[0, i].wait_recv()
    ec = {}
    w = values_along_z(1)
    zv[0, 0:2] = (w[0:2] + up(dv2[0, 0]) + up(dv2[0, 1])).astype(BF16)
    zv[0, 2:4] = w[2:4].astype(BF16)
    ec[0] = send(zv.at[0], fev.at[0], yp)
    w = values_along_z(2)
    zv[1, 0:2] = w[0:2].astype(BF16)
    zv[1, 2:4] = (w[2:4] + up(dv2[1, 0]) + up(dv2[1, 1])).astype(BF16)
    ec[1] = send(zv.at[1], fev.at[1], ym)

    for i in (4, 6):
        kc[i].wait_recv()

    def keys_along_y(q):
        return up(ak[3, q]) + up(fk[0, q]) + up(fk[1, q])

    for i in (14, 16, 17, 18):
        kc[i].wait_recv()
    gc = {}
    w = keys_along_y(2)
    yk[0, 0:2] = (w[0:2] + up(dk2[0, 0]) + up(dk2[0, 1])).astype(BF16)
    yk[0, 2:4] = w[2:4].astype(BF16)
    gc[0] = send(yk.at[0], fgk.at[0], zp)
    w = keys_along_y(0)
    yk[1, 0:2] = w[0:2].astype(BF16)
    yk[1, 2:4] = (w[2:4] + up(dk2[1, 0]) + up(dk2[1, 1])).astype(BF16)
    gc[1] = send(yk.at[1], fgk.at[1], zm)

    w = values_along_z(3)
    for cp in ec.values():
        cp.wait_recv()
    xs[1] = (w + up(fev[0]) + up(fev[1])).astype(BF16)
    xc = []
    for k in (2, 1, 3):
        xc.append(send(xs.at[1, around(x, k)], rx.at[1, x], xo[k - 1]))
    dq_pair.wait_recv()
    dq_out[0] = ((jnp.transpose(dqt[:, mine]) + dqr[...]) * 0.0625).astype(BF16)
    for cp in gc.values():
        cp.wait_recv()
    xs[0] = (keys_along_y(1) + up(fgk[0]) + up(fgk[1])).astype(BF16)
    for k in (2, 1, 3):
        xc.append(send(xs.at[0, around(x, k)], rx.at[0, x], xo[k - 1]))
    rx[0, x] = xs[0, x]
    rx[1, x] = xs[1, x]
    for cp in xc:
        cp.wait_recv()
    for r in (0, 1):
        dk_out[r] = up(rx[0, 2 * r]) + up(rx[0, 2 * r + 1])
        dv_out[r] = up(rx[1, 2 * r]) + up(rx[1, 2 * r + 1])
    for cp in started[-SENDS:]:
        cp.wait_send()
    assert len(started) == COPIES, len(started)


def leave(a, b, c, a_out, b_out, c_out, sem):
    moves = [pltpu.make_async_copy(src, dst, sem.at[i]) for i, (src, dst) in enumerate(((a, a_out), (b, b_out), (c, c_out)))]
    for cp in moves:
        cp.start()
    for cp in moves:
        cp.wait()


def per_device(queries, keys, values, d_out, doc_lengths, fold_order):
    hbm = pl.BlockSpec(memory_space=pl.ANY)
    vmem = pl.BlockSpec(memory_space=pltpu.VMEM)
    smem = pl.BlockSpec(memory_space=pltpu.SMEM)

    def vm(*shape, dtype=BF16):
        return pltpu.VMEM(shape, dtype)

    grads = pl.pallas_call(
        kernel,
        out_shape=(
            pltpu.VMEM((1, 512, 256), BF16),
            pltpu.VMEM((2, 32, 256), F32),
            pltpu.VMEM((2, 32, 256), F32),
        ),
        in_specs=[smem, smem, hbm, hbm, hbm, hbm],
        out_specs=(vmem, vmem, vmem),
        scratch_shapes=[
            vm(1024, 256),
            vm(1024, 256),
            vm(1024, 256),
            vm(256, 1024),
            vm(256, 1024),
            vm(4, 2, 512, 256),
            vm(4, 512, 1024, dtype=F32),
            vm(4, 512, 1024, dtype=F32),
            vm(8, 1024, dtype=F32),
            vm(8, 1024, dtype=F32),
            vm(4, 512, 1024),
            vm(256, 1024, dtype=F32),
            vm(512, 256, dtype=F32),
            vm(512, 256, dtype=F32),
            vm(4, 4, 4, 32, 256),
            vm(4, 4, 4, 32, 256),
            vm(2, 4, 2, 32, 256),
            vm(2, 4, 4, 32, 256),
            vm(2, 2, 2, 32, 256),
            vm(2, 4, 2, 32, 256),
            vm(2, 4, 4, 32, 256),
            vm(2, 2, 2, 32, 256),
            vm(2, 4, 32, 256),
            vm(2, 4, 32, 256),
            vm(2, 4, 32, 256),
            vm(2, 4, 32, 256),
            vm(2, 4, 32, 256),
            vm(2, 4, 32, 256),
            pltpu.SemaphoreType.DMA((4,)),
            pltpu.SemaphoreType.DMA((SENDS,)),
            pltpu.SemaphoreType.DMA((COPIES,)),
        ],
        compiler_params=pltpu.CompilerParams(
            collective_id=0, has_side_effects=True, vmem_limit_bytes=66600000
        ),
    )(doc_lengths, fold_order, queries, keys, values, d_out)
    return pl.pallas_call(
        leave,
        out_shape=tuple(jax.ShapeDtypeStruct(g.shape, g.dtype) for g in grads),
        in_specs=[vmem] * 3,
        out_specs=(hbm,) * 3,
        scratch_shapes=[pltpu.SemaphoreType.DMA((3,))],
        compiler_params=pltpu.CompilerParams(vmem_limit_bytes=1024 * 1024),
    )(*grads)


def solution(mesh):
    in_specs = (
        P("head", "seq", None),
        P(None, "seq", None),
        P(None, "seq", None),
        P("head", "seq", None),
        P(),
        P(),
    )
    out_specs = (
        P("head", "seq", None),
        P(None, ("seq", "head"), None),
        P(None, ("seq", "head"), None),
    )
    return jax.shard_map(
        per_device, mesh=mesh, in_specs=in_specs, out_specs=out_specs, check_vma=False
    )
```
